128 devices in a mesh: row: 8 (over z, core), col: 16 (over y, x).
Axes of the slice: x: 4, y: 4, z: 4, core: 2. Of those that a mesh axis runs over, the one named last changes fastest.
Arguments:
- coefs: float32 [2, 1536, 16384], P(None, 'row', 'col'), may hold values from -600 to 600, as said below
- tilts: int32 [1536, 2], replicated, may hold values from 8 to 48
- start_basis: float32 [1536, 32], P('col'), may hold values from -6 to 6
Outputs:
- ccc: float32 [1536, 1536], P('row', 'col')
- basis: float32 [1536, 32], P('col')
The draws below stay inside these ranges and needn't reach their ends.
Inputs may be any that keep to these rules, and one draw needn't show every extreme that they name: `coefs`: real and imaginary parts are products of a particle scale, a coefficient scale and a bounded random value.
All inputs are finite; a program needn't handle non-finite values.
Results may differ from the reference program's by a relative error of at most 0.0003.
Values sent between devices are 32-bit elements; how exact they have to be, the bound alone decides.
A program may use at most 192 MiB of HBM per device.

```python
import math
import jax
import jax.numpy as jnp
from jax import lax

GRID = 32
K = 16384
P_SIZE = 1536
EIG = 32
ITERS = 4


def draw_coefs(key, part):
    first = jax.random.fold_in(key, 11)
    second = jax.random.fold_in(key, 12)
    third = jax.random.fold_in(key, 13)
    fourth = jax.random.fold_in(key, 14)
    scale_p = jnp.exp(jax.random.uniform(first, (1, P_SIZE, 1), jnp.float32) * math.log(10.0))
    scale_k = jnp.exp(jax.random.uniform(second, (1, 1, K), jnp.float32) * math.log(10.0))
    template = jnp.clip(jax.random.normal(third, (2, 1, K), jnp.float32), -5.0, 5.0)
    noise = jnp.clip(jax.random.normal(fourth, (2, P_SIZE, K), jnp.float32), -5.0, 5.0)
    weight = 0.1
    return (scale_p * scale_k * (noise + weight * template)).astype(jnp.float32)


def plant(result, own_key, smallest, largest):
    shape = result.shape
    spot = [jax.random.randint(jax.random.fold_in(own_key, axis), (), 0, shape[axis]) for axis in range(len(shape))]
    result = result.at[tuple(spot)].set(smallest)
    longest = shape.index(max(shape))
    spot[longest] = (spot[longest] + 1) % shape[longest]
    return result.at[tuple(spot)].set(largest)


def block_scale(key, dims, shards, smallest, largest):
    def one(dim, blocks):
        draws = jax.random.uniform(jax.random.fold_in(jax.random.fold_in(key, 6), dim), (blocks,), jnp.float32, smallest / len(shards), largest / len(shards))
        return jnp.repeat(jnp.exp(draws), dims[dim] // blocks).reshape((-1,) + (1,) * (len(dims) - dim - 1))

    level = one(*shards[0])
    for cut in shards[1:]:
        level = level * one(*cut)
    return level


def gaussian(stream_key, shape, width, most, pieces=(), kind=jnp.bfloat16):
    array = jax.random.normal(stream_key, shape, jnp.float32) * width
    if len(pieces) > 0:
        array = block_scale(stream_key, shape, pieces, -0.22, 0.18) * array
    return jnp.clip(array, min=-most, max=most).astype(kind)


def setup_inputs(seed: int = 0) -> dict:
    arg_keys = jax.random.split(jax.random.key(seed), 4)
    return {
        "coefs": draw_coefs(jax.random.fold_in(arg_keys[3], 71), 0),
        "tilts": plant(jax.random.randint(arg_keys[1], (P_SIZE, 2), 8, 49), jax.random.fold_in(arg_keys[1], 1), 8, 48).astype(jnp.int32),
        "start_basis": gaussian(arg_keys[2], (P_SIZE, EIG), 1.0, 6.0, ((0, 16),), jnp.float32),
    }


EPS = 1e-06
HIGH = lax.Precision.HIGHEST

def wedge(tilt_rows, wave_index):
    wave_x = jnp.abs(wave_index // (GRID * (GRID // 2)) - GRID // 2)[None, :]
    wave_z = (wave_index % GRID - GRID // 2)[None, :]
    upward = wave_z * 16 <= tilt_rows[:, 1:2] * wave_x
    downward = -wave_z * 16 <= tilt_rows[:, 0:1] * wave_x
    return jnp.where(wave_z >= 0, upward, downward).astype(jnp.float32)

def inner(left, right):
    return lax.dot_general(left.astype(jnp.float32), right.astype(jnp.float32), (((1,), (1,)), ((), ())), precision=HIGH, preferred_element_type=jnp.float32)

def reference(coefs, tilts, start_basis):
    masks = wedge(tilts, jnp.arange(K, dtype=jnp.int32))
    paired = jnp.concatenate([coefs[0] * masks, coefs[1] * masks], axis=1)
    energy = masks * (coefs[0] * coefs[0] + coefs[1] * coefs[1])
    numer = inner(paired, paired)
    intersection = inner(energy, masks)
    ccc = numer / jnp.sqrt(intersection * intersection.T + EPS)
    current = start_basis
    for step in range(ITERS):
        wide = jnp.dot(ccc.astype(jnp.float32), current.astype(jnp.float32), precision=HIGH, preferred_element_type=jnp.float32)
        gram = lax.dot_general(wide.astype(jnp.float32), wide.astype(jnp.float32), (((0,), (0,)), ((), ())), precision=HIGH, preferred_element_type=jnp.float32)
        factor = jnp.linalg.cholesky(gram)
        current = lax.linalg.triangular_solve(factor, wide, left_side=False, lower=True, transpose_a=True)
    return (ccc, current * jnp.sqrt(jnp.float32(P_SIZE)))
```

```python
import math

import jax
import jax.numpy as jnp
from jax import lax
from jax.experimental import pallas as pl
from jax.experimental.pallas import tpu as pltpu
from jax.sharding import PartitionSpec as P

GRID = 32
ITERS = 4
EPS = 1e-06
MESH = pl.DeviceIdType.MESH
F32 = jnp.float32
BF16 = jnp.bfloat16

ROWS = 192
LANES = 128
BLOCKS = 4
BLOCK = 384
PAIRS = [(a, b) for b in range(BLOCKS) for a in range(b + 1)]
TILES = 32
STACK = TILES * ROWS
COLOR = STACK // 3
SEGS = (COLOR // 4, COLOR // 16, COLOR // 64)
ORDERS = (("x", "y", "z"), ("y", "z", "x"), ("z", "x", "y"))
LOW = 8


def nt(left, right):
    return lax.dot_general(left, right, (((1,), (1,)), ((), ())), preferred_element_type=F32)


def nn(left, right):
    return lax.dot_general(left, right, (((1,), (0,)), ((), ())), preferred_element_type=F32)


def split(value):
    high = value.astype(BF16)
    return high, (value - high.astype(F32)).astype(BF16)


def kernel(
    coefs, tilts, start,
    rows_out, basis_out,
    sendbuf, own, other, x_high, x_low,
    partial, recv1, recv2, recv3, acc1, acc2, full, rden,
    table_x, table_y, table, lookup, lookup_in, first,
    c_high, c_low, vt,
    a2a_s, a2a_r, fwd_s, fwd_r, tab_s, tab_r, tf_s, tf_r, st_s, st_r,
    rs_s, rs_r, ag_s, ag_r, out_s, out_r,
):
    r = lax.axis_index("row")
    c = lax.axis_index("col")
    core = r % 2
    place = {"x": c % 4, "y": c // 4, "z": r // 2}

    def peer(axis, d):
        p = (place[axis] + d) % 4
        if axis == "x":
            return p, (r, place["y"] * 4 + p)
        if axis == "y":
            return p, (r, p * 4 + place["x"])
        return p, (p * 2 + core, c)

    partner = (place["z"] * 2 + 1 - core, c)

    def send(src, dst, ss, rs, device):
        copy = pltpu.make_async_remote_copy(
            src_ref=src, dst_ref=dst, send_sem=ss, recv_sem=rs,
            device_id=device, device_id_type=MESH,
        )
        copy.start()
        return copy

    barrier = pltpu.get_barrier_semaphore()
    for d in range(1, 8):
        pl.semaphore_signal(barrier, inc=1, device_id=((r + d) % 8, c), device_id_type=MESH)
    for axis in ("x", "y"):
        for d in range(1, 4):
            pl.semaphore_signal(barrier, inc=1, device_id=peer(axis, d)[1], device_id_type=MESH)

    mine = tilts[pl.ds(pl.multiple_of(r * ROWS, 8), ROWS), :]
    wave = c * 1024 + lax.broadcasted_iota(jnp.int32, (1, 1024), 1)
    wave_x = jnp.abs(wave // (GRID * (GRID // 2)) - GRID // 2)
    wave_z = wave % GRID - GRID // 2
    need = jnp.abs(wave_z) * 16
    limit = jnp.where(wave_z >= 0, mine[:, 1:2], mine[:, 0:1])
    masks = (need <= limit * wave_x).astype(F32)
    real = coefs[0] * masks
    imag = coefs[1] * masks
    for q in range(8):
        sendbuf[q, 0] = real[:, q * LANES : (q + 1) * LANES]
        sendbuf[q, 1] = imag[:, q * LANES : (q + 1) * LANES]
    own[r] = sendbuf[r]
    first[pl.ds(pl.multiple_of(c * 96, 8), 96), :] = jnp.zeros((96, LANES), F32)
    first[pl.ds(pl.multiple_of(c * 96, 8), 96), 0:32] = start[...]
    pl.semaphore_wait(barrier, 13)

    exchange = []
    for n, d in enumerate((2, 6, 1, 7, 3, 5, 4)):
        p = (r + d) % 8
        exchange.append((d, send(sendbuf.at[p], own.at[r], a2a_s.at[n], a2a_r.at[n], (p, c))))
    forward = [send(own.at[r], other.at[r], fwd_s.at[0], fwd_r.at[0], partner)]

    energy = real * real + imag * imag
    slope = lax.broadcasted_iota(jnp.int32, (LANES, 1), 0)
    side = jnp.where(slope < 64, 1, 0)
    below = need <= (slope % 64 + LOW) * wave_x
    positive = jnp.where(wave_z >= 0, 1, 0)
    pattern = jnp.where(below & (side == positive), 1.0, 0.0).astype(BF16)
    high, rest = split(energy)
    rest32 = energy - high.astype(F32)
    middle, low = split(rest32)
    sums = nt(high, pattern) + nt(middle, pattern) + nt(low, pattern)

    def ring_sum(buffer, value, axis, base):
        buffer[place[axis]] = value
        copies = []
        for d in range(1, 4):
            copies.append(send(
                buffer.at[place[axis]], buffer.at[place[axis]],
                tab_s.at[base + d - 1], tab_r.at[base + d - 1], peer(axis, d)[1],
            ))
        return copies

    copies = ring_sum(table_x, sums, "x", 0)
    mine_rows = pl.ds(pl.multiple_of(c * 96, 8), 96)
    starts = [
        send(first.at[mine_rows], first.at[mine_rows], st_s.at[d - 1], st_r.at[d - 1], peer("x", d)[1])
        for d in range(1, 4)
    ]
    column = lax.broadcasted_iota(jnp.int32, (1536, LANES), 1)
    chosen = (column == tilts[:, 1:2] - LOW) | (column == tilts[:, 0:1] - LOW + 64)
    chosen = jnp.where(chosen, 1.0, 0.0).astype(BF16)
    lookup[:, 0:LANES] = chosen
    lookup[:, LANES:] = chosen
    for copy in copies:
        copy.wait()
    total = (table_x[0] + table_x[1]) + (table_x[2] + table_x[3])
    copies = ring_sum(table_y, total, "y", 3)
    for copy in starts:
        copy.wait()
    mine_rows = pl.ds(pl.multiple_of(place["y"] * 384, 8), 384)
    starts = [
        send(first.at[mine_rows], first.at[mine_rows], st_s.at[d + 2], st_r.at[d + 2], peer("y", d)[1])
        for d in range(1, 4)
    ]
    for copy in copies:
        copy.wait()
    total = (table_y[0] + table_y[1]) + (table_y[2] + table_y[3])
    table[r] = total
    copies = [
        send(table.at[r], table.at[r], tab_s.at[5 + d], tab_r.at[5 + d], peer("z", d)[1])
        for d in range(1, 4)
    ]
    table_forward = [send(table.at[r], table.at[r], tf_s.at[0], tf_r.at[0], partner)]
    for copy in starts:
        copy.wait()

    for n, (d, copy) in enumerate(exchange):
        copy.wait()
        source = (r - d + 8) % 8
        forward.append(send(own.at[source], other.at[source], fwd_s.at[n + 1], fwd_r.at[n + 1], partner))
    for copy in forward:
        copy.wait()
    for source in range(8):
        for part, ref in enumerate((own, other)):
            for k in range(2):
                at = (2 * part + k) * LANES
                high, low = split(ref[source, k])
                x_high[source * ROWS : (source + 1) * ROWS, at : at + LANES] = high
                x_low[source * ROWS : (source + 1) * ROWS, at : at + LANES] = low

    reduce = {}

    def scatter(color, phase, source):
        axis = ORDERS[color][phase]
        size = SEGS[phase]
        target = (recv1, recv2, recv3)[phase]
        copies = []
        for d in range(1, 4):
            p, device = peer(axis, d)
            n = (color * 3 + phase) * 3 + d - 1
            copies.append(send(
                source.at[pl.ds(pl.multiple_of(p * size, 8), size)],
                target.at[color, d - 1], rs_s.at[n], rs_r.at[n], device,
            ))
        reduce[color, phase] = copies

    def gather_sum(color, phase, source):
        for copy in reduce[color, phase]:
            copy.wait()
        size = SEGS[phase]
        target = (recv1, recv2, recv3)[phase]
        at = place[ORDERS[color][phase]] * size
        value = source[pl.ds(pl.multiple_of(at, 8), size), :]
        return (value + target[color, 0]) + (target[color, 1] + target[color, 2])

    partial[30 * ROWS :, :] = jnp.zeros((2 * ROWS, LANES), F32)
    pair = 0
    begun = 0
    for b in range(BLOCKS):
        right_high = x_high[b * BLOCK : (b + 1) * BLOCK, :]
        right_low = x_low[b * BLOCK : (b + 1) * BLOCK, :]
        picks = [pl.ds(pl.multiple_of(a * BLOCK + core * ROWS, 8), ROWS) for a in range(b + 1)]
        left_high = jnp.concatenate([x_high[pick, :] for pick in picks], axis=0)
        left_low = jnp.concatenate([x_low[pick, :] for pick in picks], axis=0)
        product = nt(left_high, right_high) + nt(left_high, right_low) + nt(left_low, right_high)
        for a in range(b + 1):
            for k in range(3):
                at = (3 * pair + k) * ROWS
                partial[at : at + ROWS, :] = product[a * ROWS : (a + 1) * ROWS, k * LANES : (k + 1) * LANES]
            pair += 1
        done = pair * 3 * ROWS if b < BLOCKS - 1 else STACK
        while begun < 3 and (begun + 1) * COLOR <= done:
            scatter(begun, 0, partial.at[begun * COLOR : (begun + 1) * COLOR])
            begun += 1

    for d, copy in zip(range(1, 4), copies):
        copy.wait()
        source = ((place["z"] - d + 4) % 4) * 2 + core
        table_forward.append(send(table.at[source], table.at[source], tf_s.at[d], tf_r.at[d], partner))
    for copy in table_forward:
        copy.wait()
    for source in range(8):
        high, low = split(table[source])
        lookup_in[source * ROWS : (source + 1) * ROWS, 0:LANES] = high
        lookup_in[source * ROWS : (source + 1) * ROWS, LANES:] = low

    def norms(pair, a, b):
        def body(half, carry):
            pick = pl.ds(pl.multiple_of(a * BLOCK + half * ROWS, 8), ROWS)
            one = nt(lookup_in[pick, :], lookup[b * BLOCK : (b + 1) * BLOCK, :])
            two = nt(lookup[pick, :], lookup_in[b * BLOCK : (b + 1) * BLOCK, :])
            value = lax.rsqrt(one * two + EPS)
            for k in range(3):
                at = (3 * pair + k) * ROWS
                rden[half, at : at + ROWS, :] = value[:, k * LANES : (k + 1) * LANES]
            return carry

        lax.fori_loop(0, 2, body, 0)

    for pair, (a, b) in enumerate(PAIRS):
        norms(pair, a, b)

    for color in range(3):
        acc1[color] = gather_sum(color, 0, partial.at[color * COLOR : (color + 1) * COLOR])
        scatter(color, 1, acc1.at[color])
    for color in range(3):
        acc2[color] = gather_sum(color, 1, acc1.at[color])
        scatter(color, 2, acc2.at[color])

    spread = {}

    def region(color, phase):
        order = ORDERS[color]
        at = color * COLOR
        for step in range(phase + 1):
            at = at + place[order[step]] * SEGS[step]
        return at

    def broadcast(color, phase):
        piece = full.at[core, pl.ds(pl.multiple_of(region(color, phase), 8), SEGS[phase])]
        copies = []
        for d in range(1, 4):
            n = (color * 3 + phase) * 3 + d - 1
            copies.append(send(piece, piece, ag_s.at[n], ag_r.at[n], peer(ORDERS[color][phase], d)[1]))
        spread[color, phase] = copies

    for color in range(3):
        value = gather_sum(color, 2, acc2.at[color])
        full[core, pl.ds(pl.multiple_of(region(color, 2), 8), SEGS[2]), :] = value
        broadcast(color, 2)
    for phase in (1, 0):
        for color in range(3):
            for copy in spread[color, phase + 1]:
                copy.wait()
            broadcast(color, phase)
    last = []
    for color in range(3):
        for d in range(4):
            if d > 0:
                spread[color, 0][d - 1].wait()
            at = color * COLOR + ((place[ORDERS[color][0]] - d + 4) % 4) * SEGS[0]
            piece = full.at[core, pl.ds(pl.multiple_of(at, 8), SEGS[0])]
            n = color * 4 + d
            last.append(send(piece, piece, out_s.at[n], out_r.at[n], partner))
    for copy in last:
        copy.wait()

    for pair, (a, b) in enumerate(PAIRS):
        for k in range(3):
            at = (3 * pair + k) * ROWS
            halves = [full[half, at : at + ROWS, :] * rden[half, at : at + ROWS, :] for half in range(2)]
            value = jnp.concatenate(halves, axis=0)
            lane = b * BLOCK + k * LANES
            high, low = split(value)
            c_high[a * BLOCK : (a + 1) * BLOCK, lane : lane + LANES] = high
            c_low[a * BLOCK : (a + 1) * BLOCK, lane : lane + LANES] = low
            if a < b:
                high, low = split(value.T)
                c_high[lane : lane + LANES, a * BLOCK : (a + 1) * BLOCK] = high
                c_low[lane : lane + LANES, a * BLOCK : (a + 1) * BLOCK] = low
    pick = pl.ds(pl.multiple_of(r * ROWS, 16), ROWS)
    rows_out[...] = c_high[pick, :].astype(F32) + c_low[pick, :].astype(F32)

    vt[...] = first[...].T[0:32, :]
    row_of = lax.broadcasted_iota(jnp.int32, (32, 32), 0)
    column_of = lax.broadcasted_iota(jnp.int32, (32, 32), 1)

    def iterate(step, carry):
        v_high, v_low = split(vt[...])
        both = jnp.concatenate([v_high, v_low], axis=0)
        wide = nn(both, c_high[...])
        wide = wide[0:32] + wide[32:64] + nn(v_high, c_low[...])
        w_high, w_low = split(wide)
        gram = nt(w_high, w_high) + (nt(w_high, w_low) + nt(w_low, w_high))
        inverse = jnp.where(row_of == column_of, 1.0, 0.0).astype(F32)
        for j in range(32):
            factor = gram[:, j : j + 1] * (1.0 / gram[j : j + 1, j : j + 1])
            factor = jnp.where(row_of[:, 0:1] > j, factor, 0.0)
            gram, inverse = (
                gram - factor * gram[j : j + 1, :],
                inverse - factor * inverse[j : j + 1, :],
            )
        pivots = jnp.sum(jnp.where(row_of == column_of, gram, 0.0), axis=1, keepdims=True)
        inverse = inverse * lax.rsqrt(pivots)
        i_high, i_low = split(inverse)
        vt[...] = nn(i_high, w_high) + (nn(i_high, w_low) + nn(i_low, w_high))
        return carry

    lax.fori_loop(0, ITERS, iterate, 0)
    basis_out[...] = vt[...] * math.sqrt(1536)


def local(coefs, tilts, start_basis):
    vmem = pl.BlockSpec(memory_space=pltpu.VMEM)
    dma = pltpu.SemaphoreType.DMA
    rows, basis = pl.pallas_call(
        kernel,
        out_shape=(
            jax.ShapeDtypeStruct((ROWS, 1536), F32),
            jax.ShapeDtypeStruct((32, 1536), F32),
        ),
        in_specs=[vmem] * 3,
        out_specs=(vmem, vmem),
        scratch_shapes=[
            pltpu.VMEM((8, 2, ROWS, LANES), F32),
            pltpu.VMEM((8, 2, ROWS, LANES), F32),
            pltpu.VMEM((8, 2, ROWS, LANES), F32),
            pltpu.VMEM((1536, 512), BF16),
            pltpu.VMEM((1536, 512), BF16),
            pltpu.VMEM((STACK, LANES), F32),
            pltpu.VMEM((3, 3, SEGS[0], LANES), F32),
            pltpu.VMEM((3, 3, SEGS[1], LANES), F32),
            pltpu.VMEM((3, 3, SEGS[2], LANES), F32),
            pltpu.VMEM((3, SEGS[0], LANES), F32),
            pltpu.VMEM((3, SEGS[1], LANES), F32),
            pltpu.VMEM((2, STACK, LANES), F32),
            pltpu.VMEM((2, STACK, LANES), F32),
            pltpu.VMEM((4, ROWS, LANES), F32),
            pltpu.VMEM((4, ROWS, LANES), F32),
            pltpu.VMEM((8, ROWS, LANES), F32),
            pltpu.VMEM((1536, 2 * LANES), BF16),
            pltpu.VMEM((1536, 2 * LANES), BF16),
            pltpu.VMEM((1536, LANES), F32),
            pltpu.VMEM((1536, 1536), BF16),
            pltpu.VMEM((1536, 1536), BF16),
            pltpu.VMEM((32, 1536), F32),
            dma((7,)), dma((7,)), dma((8,)), dma((8,)),
            dma((9,)), dma((9,)), dma((4,)), dma((4,)), dma((6,)), dma((6,)),
            dma((27,)), dma((27,)), dma((27,)), dma((27,)), dma((12,)), dma((12,)),
        ],
        compiler_params=pltpu.CompilerParams(
            collective_id=0, has_side_effects=True, vmem_limit_bytes=62 << 20
        ),
        name="whole",
    )(coefs, tilts, start_basis)
    col = lax.axis_index("col")
    block = lax.dynamic_slice_in_dim(rows, col * 96, 96, 1)
    current = lax.dynamic_slice_in_dim(basis, col * 96, 96, 1).T
    return block, current


def solution(mesh):
    in_specs = (P(None, "row", "col"), P(), P("col", None))
    out_specs = (P("row", "col"), P("col", None))
    return jax.shard_map(local, mesh=mesh, in_specs=in_specs, out_specs=out_specs, check_vma=False)
```

```python
import math

import jax
import jax.numpy as jnp
from jax import lax
from jax.experimental import pallas as pl
from jax.experimental.pallas import tpu as pltpu
from jax.sharding import PartitionSpec as P

GRID = 32
ITERS = 4
EPS = 1e-06
MESH = pl.DeviceIdType.MESH
F32 = jnp.float32
BF16 = jnp.bfloat16

ROWS = 192
PART = 96
N = 128
LOW = 8
WIDE = 6

SLOTS = ([], [])
for J in range(WIDE - 1, -1, -1):
    for half in range(2):
        odd = (half + J) % 2
        SLOTS[half].extend((2 * i + odd, 2 * J + k) for i in range(J) for k in range(2))
        SLOTS[half].append((2 * J + odd, 2 * J + 1))
    if J % 2 == 0:
        SLOTS[0].append((2 * J, 2 * J))
        SLOTS[1].append((2 * J + 2, 2 * J + 2))
TILES = len(SLOTS[0])
ORDERS = (("x", "y", "z"), ("y", "z", "x"), ("z", "x", "y"))
STREAMS = [(7 * s, 7, ORDERS[s]) for s in range(3)] + [(21 + 6 * s, 6, ORDERS[s]) for s in range(3)]
MOST = 7
PANEL = 16


def nt(left, right):
    return lax.dot_general(left, right, (((1,), (1,)), ((), ())), preferred_element_type=F32)


def nn(left, right):
    return lax.dot_general(left, right, (((1,), (0,)), ((), ())), preferred_element_type=F32)


def split(value):
    high = value.astype(BF16)
    return high, (value - high.astype(F32)).astype(BF16)


def rows_at(at, size):
    return pl.ds(pl.multiple_of(at, 8), size)


def lower_inverse(gram):
    row_of = lax.broadcasted_iota(jnp.int32, (32, 32), 0)
    column_of = lax.broadcasted_iota(jnp.int32, (32, 32), 1)

    def everywhere(value):
        return jnp.broadcast_to(value, (32, 32))

    inverse = jnp.where(row_of == column_of, 1.0, 0.0).astype(F32)
    pivots = jnp.ones((32, 32), F32)
    for j in range(0, 32, PANEL):
        columns = [everywhere(gram[:, j + q : j + q + 1]) for q in range(PANEL)]
        for p in range(PANEL):
            at = slice(j + p, j + p + 1)
            pivot = everywhere(columns[p][at, :])
            pivots = jnp.where(row_of == j + p, pivot, pivots)
            factor = jnp.where(row_of > j + p, columns[p] * (1.0 / pivot), 0.0)
            for q in range(p + 1, PANEL):
                columns[q] = columns[q] - factor * everywhere(columns[q][at, :])
            gram = gram - factor * everywhere(gram[at, :])
            inverse = inverse - factor * everywhere(inverse[at, :])
    return inverse * lax.rsqrt(pivots)


def kernel(
    coefs, tilts, start,
    block_out, basis_out,
    held, own, other, x_high, x_low, masks, chosen, corner,
    partial, recv_a, recv_b, recv_c, acc, full, rden,
    table_x, table_y, table, lookup, lookup_in, first,
    c_high, c_low, wt,
    held_s, a2a_s, a2a_r, fwd_s, fwd_r, tab_s, tab_r, tf_s, tf_r, st_s, st_r,
    ra_s, ra_r, rb_s, rb_r, rc_s, rc_r, gb_s, gb_r, ga_s, ga_r, out_s, out_r,
):
    r = lax.axis_index("row")
    c = lax.axis_index("col")
    core = r % 2
    mate = r + 1 - 2 * core
    place = {"x": c % 4, "y": c // 4, "z": r // 2}

    def peer(axis, d):
        p = (place[axis] + d) % 4
        if axis == "x":
            return p, (r, place["y"] * 4 + p)
        if axis == "y":
            return p, (r, p * 4 + place["x"])
        return p, (p * 2 + core, c)

    partner = (mate, c)

    def send(src, dst, ss, rs, device):
        copy = pltpu.make_async_remote_copy(
            src_ref=src, dst_ref=dst, send_sem=ss, recv_sem=rs,
            device_id=device, device_id_type=MESH,
        )
        copy.start()
        return copy

    barrier = pltpu.get_barrier_semaphore()
    for d in range(1, 8):
        pl.semaphore_signal(barrier, inc=1, device_id=((r + d) % 8, c), device_id_type=MESH)
    for axis in ("x", "y"):
        for d in range(1, 4):
            pl.semaphore_signal(barrier, inc=1, device_id=peer(axis, d)[1], device_id_type=MESH)
    locals_ = [pltpu.make_async_copy(coefs, held, held_s.at[0])]
    mine = pl.ds(pl.multiple_of(r * N, N), N)
    locals_.append(pltpu.make_async_copy(coefs.at[:, :, mine], own.at[r], held_s.at[1]))
    for copy in locals_:
        copy.start()
    corner[...] = jnp.zeros((N, N), F32)
    corner[0:32, 0:PART] = start[...]
    first[rows_at(c * PART, PART), :] = corner[...].T[0:PART, :]
    pl.semaphore_wait(barrier, 13)

    exchange = ([], [])
    forward = ([], [])
    for part in range(2):
        for n, d in enumerate((2, 6, 1, 7, 3, 5, 4)):
            p = (r + d) % 8
            n = 7 * part + n
            exchange[part].append((d, send(
                coefs.at[part, :, pl.ds(pl.multiple_of(p * N, N), N)],
                own.at[r, part], a2a_s.at[n], a2a_r.at[n], (p, c),
            )))
        forward[part].append(send(
            coefs.at[part, :, mine], other.at[r, part], fwd_s.at[8 * part], fwd_r.at[8 * part], partner,
        ))
    own_rows = rows_at(c * PART, PART)
    starts = [
        send(first.at[own_rows], first.at[own_rows], st_s.at[d - 1], st_r.at[d - 1], peer("x", d)[1])
        for d in range(1, 4)
    ]

    low_side = tilts[0:1, :]
    high_side = tilts[1:2, :]
    line = lax.broadcasted_iota(jnp.int32, (N, 1536), 0)
    picked = (line == high_side - LOW) | (line == low_side - LOW + 64)
    picked = jnp.where(picked, 1.0, 0.0)
    picked = jnp.where(line == 126, low_side.astype(F32), picked)
    picked = jnp.where(line == 127, high_side.astype(F32), picked)
    chosen[...] = picked.T
    column = lax.broadcasted_iota(jnp.int32, (1536, N), 1)
    one_hot = jnp.where(column < 126, chosen[...], 0.0).astype(BF16)
    lookup[:, 0:N] = one_hot
    lookup[:, N:] = one_hot

    def waves(at, count):
        wave = at + lax.broadcasted_iota(jnp.int32, (1, count), 1)
        wave_x = jnp.abs(wave // (GRID * (GRID // 2)) - GRID // 2).astype(F32)
        wave_z = wave % GRID - GRID // 2
        return wave_x, wave_z >= 0, (jnp.abs(wave_z) * 16).astype(F32)

    def wedge(pick, wave):
        wave_x, upward, need = wave
        limit = jnp.where(upward, chosen[pick, 127:128], chosen[pick, 126:127])
        return jnp.where(need <= limit * wave_x, 1.0, 0.0)

    for side, position in enumerate((r, mate)):
        wave = waves(c * 1024 + position * N, N)
        for source in range(8):
            pick = pl.ds(source * ROWS, ROWS)
            masks[pick, side * N : (side + 1) * N] = wedge(pick, wave)

    wave = waves(c * 1024, 1024)
    wave_x, upward, need = wave
    own_mask = wedge(rows_at(r * ROWS, ROWS), wave)
    for copy in locals_:
        copy.wait()
    real, imag = held[0] * own_mask, held[1] * own_mask
    energy = real * real + imag * imag
    slope = lax.broadcasted_iota(jnp.int32, (N, 1), 0)
    below = need <= (slope % 64 + LOW).astype(F32) * wave_x
    side = jnp.where(slope < 64, 1, 0) == jnp.where(upward, 1, 0)
    pattern = jnp.where(below & side, 1.0, 0.0).astype(BF16)
    high = energy.astype(BF16)
    middle, low = split(energy - high.astype(F32))
    sums = nt(high, pattern) + nt(middle, pattern) + nt(low, pattern)

    def ring_send(buffer, value, axis, base):
        buffer[place[axis]] = value
        return [
            send(
                buffer.at[place[axis]], buffer.at[place[axis]],
                tab_s.at[base + d - 1], tab_r.at[base + d - 1], peer(axis, d)[1],
            )
            for d in range(1, 4)
        ]

    copies = ring_send(table_x, sums, "x", 0)
    for copy in starts:
        copy.wait()
    own_rows = rows_at(place["y"] * 4 * PART, 4 * PART)
    starts = [
        send(first.at[own_rows], first.at[own_rows], st_s.at[d + 2], st_r.at[d + 2], peer("y", d)[1])
        for d in range(1, 4)
    ]
    for copy in copies:
        copy.wait()
    copies = ring_send(table_y, (table_x[0] + table_x[1]) + (table_x[2] + table_x[3]), "y", 3)

    def arrive(part):
        for n, (d, copy) in enumerate(exchange[part]):
            copy.wait()
            source = (r - d + 8) % 8
            n = 8 * part + n + 1
            forward[part].append(send(
                own.at[source, part], other.at[source, part], fwd_s.at[n], fwd_r.at[n], partner,
            ))
        for side, ref in enumerate((own, other)):
            if side == 1:
                for copy in forward[part]:
                    copy.wait()
            for source in range(8):
                pick = pl.ds(source * ROWS, ROWS)
                lane = slice(side * N, (side + 1) * N)
                high, low = split(ref[source, part] * masks[pick, lane])
                x_high[part, pick, lane] = high
                x_low[part, pick, lane] = low

    started = {}

    def scatter(s, source, buffer, size, axis, ss, rs):
        copies = []
        for d in range(1, 4):
            p, device = peer(axis, d)
            n = 3 * s + d - 1
            copies.append(send(
                source.at[rows_at(p * size, size)],
                buffer.at[s, d - 1, pl.ds(0, size)], ss.at[n], rs.at[n], device,
            ))
        return copies

    def scatter_a(s):
        at, count, order = STREAMS[s]
        source = partial.at[pl.ds(at * N, count * N)]
        started["a", s] = scatter(s, source, recv_a, count * 32, order[0], ra_s, ra_r)

    def products(part):
        at = 0
        stream = 0
        extra = None
        for J in range(WIDE - 1, -1, -1):
            odd = (core + J) % 2
            right_high = x_high[part, J * 2 * N : (J + 1) * 2 * N, :]
            right_low = x_low[part, J * 2 * N : (J + 1) * 2 * N, :]
            picks = [pl.ds(pl.multiple_of((2 * i + odd) * N, N), N) for i in range(J + 1)]
            left_high = jnp.concatenate([x_high[part, pick, :] for pick in picks], axis=0)
            left_low = jnp.concatenate([x_low[part, pick, :] for pick in picks], axis=0)
            product = nt(left_high, right_high) + nt(left_high, right_low) + nt(left_low, right_high)
            tiles = [product[i * N : (i + 1) * N, k * N : (k + 1) * N] for i in range(J + 1) for k in range(2)]
            spare = tiles.pop(2 * J)
            if J % 2 == 1:
                extra = spare
            else:
                tiles.append(jnp.where(core == 0, spare, extra))
            for tile in tiles:
                pick = slice(at * N, (at + 1) * N)
                if part == 0:
                    partial[pick, :] = tile
                else:
                    partial[pick, :] += tile
                at += 1
            if part == 1:
                while stream < 6 and STREAMS[stream][0] + STREAMS[stream][1] <= at:
                    scatter_a(stream)
                    stream += 1

    arrive(0)
    products(0)
    for copy in copies:
        copy.wait()
    table[r] = (table_y[0] + table_y[1]) + (table_y[2] + table_y[3])
    copies = [
        send(table.at[r], table.at[r], tab_s.at[5 + d], tab_r.at[5 + d], peer("z", d)[1])
        for d in range(1, 4)
    ]
    table_forward = [send(table.at[r], table.at[r], tf_s.at[0], tf_r.at[0], partner)]
    for copy in starts:
        copy.wait()
    arrive(1)
    products(1)

    for d, copy in zip(range(1, 4), copies):
        copy.wait()
        source = ((place["z"] - d + 4) % 4) * 2 + core
        table_forward.append(send(table.at[source], table.at[source], tf_s.at[d], tf_r.at[d], partner))
    for copy in table_forward:
        copy.wait()
    for source in range(8):
        high, low = split(table[source])
        lookup_in[source * ROWS : (source + 1) * ROWS, 0:N] = high
        lookup_in[source * ROWS : (source + 1) * ROWS, N:] = low

    def norms(half):
        at = 0
        extra = None
        for J in range(WIDE - 1, -1, -1):
            odd = (half + J) % 2
            right = slice(J * 2 * N, (J + 1) * 2 * N)
            picks = [slice((2 * i + odd) * N, (2 * i + odd + 1) * N) for i in range(J + 1)]
            sums_in = jnp.concatenate([lookup_in[pick, :] for pick in picks], axis=0)
            select = jnp.concatenate([lookup[pick, :] for pick in picks], axis=0)
            value = lax.rsqrt(nt(sums_in, lookup[right, :]) * nt(select, lookup_in[right, :]) + EPS)
            tiles = [value[i * N : (i + 1) * N, k * N : (k + 1) * N] for i in range(J + 1) for k in range(2)]
            spare = tiles.pop(2 * J)
            if odd == 0:
                extra = spare
            if J % 2 == 0:
                tiles.append(extra)
            for tile in tiles:
                rden[half, at * N : (at + 1) * N, :] = tile
                at += 1

    for half in range(2):
        norms(half)

    def scatter_b(s):
        count, order = STREAMS[s][1:]
        size = count * 32
        for copy in started["a", s]:
            copy.wait()
        pick = rows_at(STREAMS[s][0] * N + place[order[0]] * size, size)
        got = [recv_a[s, n, 0:size, :] for n in range(3)]
        acc[s, 0:size, :] = (partial[pick, :] + got[0]) + (got[1] + got[2])
        started["b", s] = scatter(s, acc.at[s], recv_b, count * 8, order[1], rb_s, rb_r)

    def spread_c(s):
        count, order = STREAMS[s][1:]
        size = count * 8
        for copy in started["b", s]:
            copy.wait()
        got = [recv_b[s, n, 0:size, :] for n in range(3)]
        value = (acc[s, rows_at(place[order[1]] * size, size), :] + got[0]) + (got[1] + got[2])
        here = place[order[2]]
        recv_c[s, here, 0:size, :] = value
        piece = recv_c.at[s, here, pl.ds(0, size)]
        started["c", s] = [
            send(piece, piece, rc_s.at[3 * s + d - 1], rc_r.at[3 * s + d - 1], peer(order[2], d)[1])
            for d in range(1, 4)
        ]

    def gather_b(s):
        at, count, order = STREAMS[s]
        size = count * 8
        for copy in started["c", s]:
            copy.wait()
        got = [recv_c[s, n, 0:size, :] for n in range(4)]
        pick = rows_at(at * N + (place[order[0]] * 4 + place[order[1]]) * size, size)
        full[core, pick, :] = (got[0] + got[1]) + (got[2] + got[3])
        piece = full.at[core, pick]
        started["B", s] = [
            send(piece, piece, gb_s.at[3 * s + d - 1], gb_r.at[3 * s + d - 1], peer(order[1], d)[1])
            for d in range(1, 4)
        ]

    def pass_on(s, d, order, at, size):
        piece = full.at[core, rows_at(at * N + (place[order[0]] - d + 4) % 4 * size, size)]
        return send(piece, piece, out_s.at[4 * s + d], out_r.at[4 * s + d], partner)

    def gather_a(s):
        at, count, order = STREAMS[s]
        size = count * 32
        for copy in started["B", s]:
            copy.wait()
        piece = full.at[core, rows_at(at * N + place[order[0]] * size, size)]
        started["A", s] = [
            send(piece, piece, ga_s.at[3 * s + d - 1], ga_r.at[3 * s + d - 1], peer(order[0], d)[1])
            for d in range(1, 4)
        ]
        started["out", s] = [pass_on(s, 0, order, at, size)]

    def finish(s):
        at, count, order = STREAMS[s]
        for d in (1, 3, 2):
            started["A", s][d - 1].wait()
            started["out", s].append(pass_on(s, d, order, at, count * 32))

    def assemble(s):
        at, count, order = STREAMS[s]
        for copy in started["out", s]:
            copy.wait()
        for tile in range(at, at + count):
            for half in range(2):
                A, B = SLOTS[half][tile]
                pick = slice(tile * N, (tile + 1) * N)
                value = full[half, pick, :] * rden[half, pick, :]
                high, low = split(value)
                down, across = slice(A * N, (A + 1) * N), slice(B * N, (B + 1) * N)
                c_high[down, across] = high
                c_low[down, across] = low
                if A < B:
                    high, low = split(value.T)
                    c_high[across, down] = high
                    c_low[across, down] = low

    early, late = (0, 1, 2), (3, 4, 5)
    for s in early:
        scatter_b(s)
    for s in early:
        spread_c(s)
    for s in late:
        scatter_b(s)
    for s in early:
        gather_b(s)
    for s in late:
        spread_c(s)
    for s in early:
        gather_a(s)
    for s in late:
        gather_b(s)
    for s in late:
        gather_a(s)
    for s in early:
        finish(s)
    for s in early:
        assemble(s)
    for s in late:
        finish(s)
    for s in late:
        assemble(s)

    def times_matrix(high, low):
        wide = nn(jnp.concatenate([high, low], axis=0), c_high[...])
        return wide[0:32] + wide[32:64] + nn(high, c_low[...])

    def gram_of(high, low):
        return nt(high, high) + (nt(high, low) + nt(low, high))

    def solved(inverse, high, low):
        inverse_high, inverse_low = split(inverse)
        return nn(inverse_high, high) + (nn(inverse_high, low) + nn(inverse_low, high))

    wt[...] = first[...].T[0:32, :]

    def iterate(step, carry):
        high, low = split(times_matrix(*split(wt[...])))
        inverse = lower_inverse(gram_of(high, low))
        wt[...] = solved(inverse, high, low)
        return carry

    lax.fori_loop(0, ITERS, iterate, 0)
    first[:, 0:32] = (wt[...] * math.sqrt(1536)).T
    basis_out[...] = first[rows_at(c * PART, PART), :].T[0:32, :]
    lane = jnp.minimum(c * PART // N, 1536 // N - 2) * N
    window = pl.ds(pl.multiple_of(lane, N), 2 * N)
    pick = pl.ds(pl.multiple_of(r * ROWS, 16), ROWS)
    block = c_high[pick, window].astype(F32) + c_low[pick, window].astype(F32)
    block = pltpu.roll(block, (2 * N - (c * PART - lane)) % (2 * N), 1)
    block_out[...] = block[:, 0:PART]


def local(coefs, tilts, start_basis):
    vmem = pl.BlockSpec(memory_space=pltpu.VMEM)
    dma = pltpu.SemaphoreType.DMA
    block, basis = pl.pallas_call(
        kernel,
        out_shape=(
            jax.ShapeDtypeStruct((ROWS, PART), F32),
            jax.ShapeDtypeStruct((32, PART), F32),
        ),
        in_specs=[pl.BlockSpec(memory_space=pltpu.HBM), vmem, vmem],
        out_specs=(vmem, vmem),
        scratch_shapes=[
            pltpu.VMEM((2, ROWS, 1024), F32),
            pltpu.VMEM((8, 2, ROWS, N), F32),
            pltpu.VMEM((8, 2, ROWS, N), F32),
            pltpu.VMEM((2, 1536, 2 * N), BF16),
            pltpu.VMEM((2, 1536, 2 * N), BF16),
            pltpu.VMEM((1536, 2 * N), F32),
            pltpu.VMEM((1536, N), F32),
            pltpu.VMEM((N, N), F32),
            pltpu.VMEM((TILES * N, N), F32),
            pltpu.VMEM((6, 3, MOST * 32, N), F32),
            pltpu.VMEM((6, 3, MOST * 8, N), F32),
            pltpu.VMEM((6, 4, MOST * 8, N), F32),
            pltpu.VMEM((6, MOST * 32, N), F32),
            pltpu.VMEM((2, TILES * N, N), F32),
            pltpu.VMEM((2, TILES * N, N), F32),
            pltpu.VMEM((4, ROWS, N), F32),
            pltpu.VMEM((4, ROWS, N), F32),
            pltpu.VMEM((8, ROWS, N), F32),
            pltpu.VMEM((1536, 2 * N), BF16),
            pltpu.VMEM((1536, 2 * N), BF16),
            pltpu.VMEM((1536, N), F32),
            pltpu.VMEM((1536, 1536), BF16),
            pltpu.VMEM((1536, 1536), BF16),
            pltpu.VMEM((32, 1536), F32),
            dma((2,)),
            dma((14,)), dma((14,)), dma((16,)), dma((16,)),
            dma((9,)), dma((9,)), dma((4,)), dma((4,)), dma((6,)), dma((6,)),
            dma((18,)), dma((18,)), dma((18,)), dma((18,)), dma((18,)), dma((18,)),
            dma((18,)), dma((18,)), dma((18,)), dma((18,)), dma((24,)), dma((24,)),
        ],
        compiler_params=pltpu.CompilerParams(
            collective_id=0, has_side_effects=True, vmem_limit_bytes=54272 << 10
        ),
        name="whole",
    )(coefs, tilts.T, start_basis.T)
    return block, basis.T


def solution(mesh):
    in_specs = (P(None, "row", "col"), P(), P("col", None))
    out_specs = (P("row", "col"), P("col", None))
    return jax.shard_map(local, mesh=mesh, in_specs=in_specs, out_specs=out_specs, check_vma=False)
```

```python
import math

import jax
import jax.numpy as jnp
from jax import lax
from jax.experimental import pallas as pl
from jax.experimental.pallas import tpu as pltpu
from jax.sharding import PartitionSpec as P

GRID = 32
ITERS = 4
EPS = 1e-06
MESH = pl.DeviceIdType.MESH
F32 = jnp.float32
BF16 = jnp.bfloat16

ROWS = 192
PART = 96
N = 128
LOW = 8
WIDE = 6

HALF = 768

SLOTS = ([], [])
for wave in ((2, 1, 0), (5, 4, 3)):
    for J in wave:
        for half in range(2):
            odd = (half + J) % 2
            SLOTS[half].extend((2 * i + odd, 2 * J + k) for i in range(J) for k in range(2))
            SLOTS[half].append((2 * J + odd, 2 * J + 1))
        if J in (0, 4, 3):
            low = J - J % 2
            SLOTS[0].append((2 * low, 2 * low))
            SLOTS[1].append((2 * low + 2, 2 * low + 2))
PLACE = [{tile: n for n, tile in enumerate(slots)} for slots in SLOTS]
TILES = len(SLOTS[0])
ORDERS = (("x", "y", "z"), ("y", "x", "z"), ("z", "x", "y"))
STREAMS = [(0, 5, ("x", "y", "z")), (5, 5, ("y", "x", "z"))]
for counts in ((4, 3, 3), (3, 4, 3), (3, 3, 3)):
    for count, order in zip(counts, ORDERS):
        STREAMS.append((STREAMS[-1][0] + STREAMS[-1][1], count, order))
MOST = 5
RELAYED = (0, 1)
HELD_BACK = (7, 10)
PANEL = 16


def nt(left, right):
    return lax.dot_general(left, right, (((1,), (1,)), ((), ())), preferred_element_type=F32)


def nn(left, right):
    return lax.dot_general(left, right, (((1,), (0,)), ((), ())), preferred_element_type=F32)


def split(value):
    high = value.astype(BF16)
    return high, (value - high.astype(F32)).astype(BF16)


def rows_at(at, size):
    return pl.ds(pl.multiple_of(at, 8), size)


def lower_inverse(gram):
    row_of = lax.broadcasted_iota(jnp.int32, (32, 32), 0)
    column_of = lax.broadcasted_iota(jnp.int32, (32, 32), 1)

    def everywhere(value):
        return jnp.broadcast_to(value, (32, 32))

    inverse = jnp.where(row_of == column_of, 1.0, 0.0).astype(F32)
    pivots = jnp.ones((32, 32), F32)
    for j in range(0, 32, PANEL):
        columns = [everywhere(gram[:, j + q : j + q + 1]) for q in range(PANEL)]
        for p in range(PANEL):
            at = slice(j + p, j + p + 1)
            pivot = everywhere(columns[p][at, :])
            pivots = jnp.where(row_of == j + p, pivot, pivots)
            factor = jnp.where(row_of > j + p, columns[p] * (1.0 / pivot), 0.0)
            for q in range(p + 1, PANEL):
                columns[q] = columns[q] - factor * everywhere(columns[q][at, :])
            gram = gram - factor * everywhere(gram[at, :])
            inverse = inverse - factor * everywhere(inverse[at, :])
    return inverse * lax.rsqrt(pivots)


def kernel(
    coefs, tilts_in, start_in,
    block_out, basis_out,
    tilts, start, held, own, other, x_high, x_low, masks, chosen, corner,
    partial, recv_a, recv_b, recv_c, acc, full, rden,
    table_x, table_y, table, lookup, lookup_in, first,
    c_high, c_low, wt,
    held_s, a2a_s, a2a_r, fwd_s, fwd_r, tab_s, tab_r, tf_s, tf_r, st_s, st_r,
    ra_s, ra_r, rb_s, rb_r, rc_s, rc_r, gb_s, gb_r, ga_s, ga_r, out_s, out_r,
):
    r = lax.axis_index("row")
    c = lax.axis_index("col")
    core = r % 2
    mate = r + 1 - 2 * core
    place = {"x": c % 4, "y": c // 4, "z": r // 2}

    def peer(axis, d):
        p = (place[axis] + d) % 4
        if axis == "x":
            return p, (r, place["y"] * 4 + p)
        if axis == "y":
            return p, (r, p * 4 + place["x"])
        return p, (p * 2 + core, c)

    partner = (mate, c)

    def send(src, dst, ss, rs, device):
        copy = pltpu.make_async_remote_copy(
            src_ref=src, dst_ref=dst, send_sem=ss, recv_sem=rs,
            device_id=device, device_id_type=MESH,
        )
        copy.start()
        return copy

    barrier = pltpu.get_barrier_semaphore()
    for d in range(1, 8):
        pl.semaphore_signal(barrier, inc=1, device_id=((r + d) % 8, c), device_id_type=MESH)
    for axis in ("x", "y"):
        for d in range(1, 4):
            pl.semaphore_signal(barrier, inc=1, device_id=peer(axis, d)[1], device_id_type=MESH)
    held_copy = pltpu.make_async_copy(coefs, held, held_s.at[0])
    held_copy.start()
    small_copies = [
        pltpu.make_async_copy(start_in, start, held_s.at[1]),
        pltpu.make_async_copy(tilts_in, tilts, held_s.at[2]),
    ]
    for copy in small_copies:
        copy.start()
    mine = pl.ds(pl.multiple_of(r * N, N), N)
    corner[...] = jnp.zeros((N, N), F32)
    small_copies[0].wait()
    corner[0:32, 0:PART] = start[...]
    here = (c % 2 * 8 + c // 2) * PART
    first[rows_at(here, PART), :] = corner[...].T[0:PART, :]
    held_copy.wait()
    pl.semaphore_wait(barrier, 13)

    cuts = (
        (slice(0, 2), pl.ds(0, PART)),
        (slice(0, 1), pl.ds(PART, PART)),
        (slice(1, 2), pl.ds(PART, PART)),
    )
    exchange = ([], [], [])
    forward = ([], [], [])
    for step, (parts, rows) in enumerate(cuts):
        for n, d in enumerate((2, 6, 1, 7, 3, 5, 4)):
            p = (r + d) % 8
            n = 7 * step + n
            exchange[step].append((d, send(
                held.at[parts, rows, pl.ds(pl.multiple_of(p * N, N), N)],
                own.at[r, parts, rows], a2a_s.at[n], a2a_r.at[n], (p, c),
            )))
        forward[step].append(send(
            held.at[parts, rows, mine], other.at[r, parts, rows],
            fwd_s.at[8 * step], fwd_r.at[8 * step], partner,
        ))
    own_rows = rows_at(here, PART)
    starts = [
        send(first.at[own_rows], first.at[own_rows], st_s.at[d - 1], st_r.at[d - 1], peer("x", d)[1])
        for d in range(1, 4)
    ]

    small_copies[1].wait()
    low_side = tilts[0:1, :]
    high_side = tilts[1:2, :]
    line = lax.broadcasted_iota(jnp.int32, (N, 1536), 0)
    picked = (line == high_side - LOW) | (line == low_side - LOW + 64)
    picked = jnp.where(picked, 1.0, 0.0)
    picked = jnp.where(line == 126, low_side.astype(F32), picked)
    picked = jnp.where(line == 127, high_side.astype(F32), picked)
    picked = picked.T
    for n in range(16):
        at = (n % 2 * 8 + n // 2) * PART
        chosen[at : at + PART, :] = picked[n * PART : (n + 1) * PART, :]
    column = lax.broadcasted_iota(jnp.int32, (1536, N), 1)
    one_hot = jnp.where(column < 126, chosen[...], 0.0).astype(BF16)
    lookup[:, 0:N] = one_hot
    lookup[:, N:] = one_hot

    def waves(at, count):
        wave = at + lax.broadcasted_iota(jnp.int32, (1, count), 1)
        wave_x = jnp.abs(wave // (GRID * (GRID // 2)) - GRID // 2).astype(F32)
        wave_z = wave % GRID - GRID // 2
        return wave_x, wave_z >= 0, (jnp.abs(wave_z) * 16).astype(F32)

    def wedge(pick, wave):
        wave_x, upward, need = wave
        limit = jnp.where(upward, chosen[pick, 127:128], chosen[pick, 126:127])
        return jnp.where(need <= limit * wave_x, 1.0, 0.0)

    for side, position in enumerate((r, mate)):
        wave = waves(c * 1024 + position * N, N)
        for source in range(8):
            pick = pl.ds(source * ROWS, ROWS)
            masks[pick, side * N : (side + 1) * N] = wedge(pick, wave)

    own[r] = held[:, :, mine]

    wave = waves(c * 1024, 1024)
    wave_x, upward, need = wave
    own_mask = jnp.concatenate(
        [wedge(rows_at(r * PART, PART), wave), wedge(rows_at(HALF + r * PART, PART), wave)], axis=0
    )
    real, imag = held[0] * own_mask, held[1] * own_mask
    energy = real * real + imag * imag
    slope = lax.broadcasted_iota(jnp.int32, (N, 1), 0)
    below = need <= (slope % 64 + LOW).astype(F32) * wave_x
    side = jnp.where(slope < 64, 1, 0) == jnp.where(upward, 1, 0)
    pattern = jnp.where(below & side, 1.0, 0.0).astype(BF16)
    high = energy.astype(BF16)
    middle, low = split(energy - high.astype(F32))
    sums = nt(high, pattern) + nt(middle, pattern) + nt(low, pattern)

    def ring_send(buffer, value, axis, base):
        buffer[place[axis]] = value
        return [
            send(
                buffer.at[place[axis]], buffer.at[place[axis]],
                tab_s.at[base + d - 1], tab_r.at[base + d - 1], peer(axis, d)[1],
            )
            for d in range(1, 4)
        ]

    copies = ring_send(table_x, sums, "x", 0)
    for copy in starts:
        copy.wait()
    starts = []
    for side in range(2):
        own_rows = rows_at(side * HALF + place["y"] * 2 * PART, 2 * PART)
        for d in range(1, 4):
            n = 3 * side + d + 2
            starts.append(send(first.at[own_rows], first.at[own_rows], st_s.at[n], st_r.at[n], peer("y", d)[1]))
    for copy in copies:
        copy.wait()
    copies = ring_send(table_y, (table_x[0] + table_x[1]) + (table_x[2] + table_x[3]), "y", 3)

    def arrive(step):
        parts, rows = cuts[step]
        for n, (d, copy) in enumerate(exchange[step]):
            copy.wait()
            source = (r - d + 8) % 8
            n = 8 * step + n + 1
            forward[step].append(send(
                own.at[source, parts, rows], other.at[source, parts, rows], fwd_s.at[n], fwd_r.at[n], partner,
            ))
        base = 0 if step == 0 else HALF
        for side, ref in enumerate((own, other)):
            if side == 1:
                for copy in forward[step]:
                    copy.wait()
            lane = slice(side * N, (side + 1) * N)
            for source in range(8):
                pick = pl.ds(base + source * PART, PART)
                mask = masks[pick, lane]
                for part in range(parts.start, parts.stop):
                    high, low = split(ref[source, part, rows, :] * mask)
                    x_high[part, pick, lane] = high
                    x_low[part, pick, lane] = low

    started = {}

    def scatter(s, source, buffer, size, axis, ss, rs):
        copies = []
        for d in range(1, 4):
            p, device = peer(axis, d)
            n = 3 * s + d - 1
            copies.append(send(
                source.at[rows_at(p * size, size)],
                buffer.at[s, d - 1, pl.ds(0, size)], ss.at[n], rs.at[n], device,
            ))
        return copies

    def scatter_a(s):
        at, count, order = STREAMS[s]
        source = partial.at[pl.ds(at * N, count * N)]
        started["a", s] = scatter(s, source, recv_a, count * 32, order[0], ra_s, ra_r)

    def product(J, part):
        odd = (core + J) % 2
        right_high = x_high[part, J * 2 * N : (J + 1) * 2 * N, :]
        right_low = x_low[part, J * 2 * N : (J + 1) * 2 * N, :]
        picks = [pl.ds(pl.multiple_of((2 * i + odd) * N, N), N) for i in range(J + 1)]
        left_high = jnp.concatenate([x_high[part, pick, :] for pick in picks], axis=0)
        left_low = jnp.concatenate([x_low[part, pick, :] for pick in picks], axis=0)
        return nt(left_high, right_high) + nt(left_high, right_low) + nt(left_low, right_high)

    def cut(J, value):
        tiles = [value[i * N : (i + 1) * N, k * N : (k + 1) * N] for i in range(J + 1) for k in range(2)]
        return tiles.pop(2 * J), tiles

    def tile_at(n):
        return slice(n * N, (n + 1) * N)

    def early_products():
        at = 0
        spares = {}
        for J in (2, 1, 0):
            spares[J], tiles = cut(J, product(J, 0) + product(J, 1))
            if J == 0:
                tiles.append(jnp.where(core == 0, spares[0], spares[1]))
            for tile in tiles:
                partial[tile_at(at), :] = tile
                at += 1
        corner[...] = spares[2]
        for s in (0, 1):
            scatter_a(s)

    def late_products(part):
        at = 10
        stream = 2
        spares = {}
        for J in (5, 4, 3):
            spares[J], tiles = cut(J, product(J, part))
            if J == 4:
                tiles.append(jnp.where(core == 0, spares[4], spares[5]))
            if J == 3:
                kept = corner[...] if part == 0 else jnp.zeros((N, N), F32)
                tiles.append(jnp.where(core == 0, kept, spares[3]))
            for tile in tiles:
                if part == 0:
                    partial[tile_at(at), :] = tile
                else:
                    partial[tile_at(at), :] += tile
                at += 1
            while part == 1 and stream < len(STREAMS) and sum(STREAMS[stream][:2]) <= at:
                if stream not in HELD_BACK:
                    scatter_a(stream)
                stream += 1

    def scatter_b(s):
        count, order = STREAMS[s][1:]
        size = count * 32
        for copy in started["a", s]:
            copy.wait()
        pick = rows_at(STREAMS[s][0] * N + place[order[0]] * size, size)
        got = [recv_a[s, n, 0:size, :] for n in range(3)]
        acc[s, 0:size, :] = (partial[pick, :] + got[0]) + (got[1] + got[2])
        started["b", s] = scatter(s, acc.at[s], recv_b, count * 8, order[1], rb_s, rb_r)

    def spread_c(s):
        count, order = STREAMS[s][1:]
        size = count * 8
        for copy in started["b", s]:
            copy.wait()
        got = [recv_b[s, n, 0:size, :] for n in range(3)]
        value = (acc[s, rows_at(place[order[1]] * size, size), :] + got[0]) + (got[1] + got[2])
        here = place[order[2]]
        recv_c[s, here, 0:size, :] = value
        piece = recv_c.at[s, here, pl.ds(0, size)]
        started["c", s] = [
            send(piece, piece, rc_s.at[3 * s + d - 1], rc_r.at[3 * s + d - 1], peer(order[2], d)[1])
            for d in range(1, 4)
        ]

    def gather_b(s):
        at, count, order = STREAMS[s]
        size = count * 8
        for copy in started["c", s]:
            copy.wait()
        got = [recv_c[s, n, 0:size, :] for n in range(4)]
        pick = rows_at(at * N + (place[order[0]] * 4 + place[order[1]]) * size, size)
        full[core, pick, :] = (got[0] + got[1]) + (got[2] + got[3])
        piece = full.at[core, pick]
        started["B", s] = [
            send(piece, piece, gb_s.at[3 * s + d - 1], gb_r.at[3 * s + d - 1], peer(order[1], d)[1])
            for d in range(1, 4)
        ]

    def piece_of(s, d, low, size):
        at, count, order = STREAMS[s]
        seg = (place[order[0]] - d + 4) % 4 * count * 32
        return full.at[core, rows_at(at * N + seg + low, size)]

    def gather_a(s):
        count, order = STREAMS[s][1:]
        for copy in started["B", s]:
            copy.wait()
        piece = piece_of(s, 0, 0, count * 32)
        started["A", s] = {
            d: send(piece, piece, ga_s.at[3 * s + d - 1], ga_r.at[3 * s + d - 1], peer(order[0], d)[1])
            for d in ((1, 3) if s in RELAYED else (1, 3, 2))
        }
        started["out", s] = []
        pass_on(s, 0)

    def pass_on(s, d):
        piece = piece_of(s, d, 0, STREAMS[s][1] * 32)
        started["out", s].append(send(piece, piece, out_s.at[4 * s + d], out_r.at[4 * s + d], partner))

    def relay(s):
        count, order = STREAMS[s][1:]
        halves = []
        for d, low in ((1, 0), (3, count * 16)):
            started["A", s][d].wait()
            piece = piece_of(s, d, low, count * 16)
            n = 3 * s + 1 if d == 1 else 33 + s
            halves.append(send(piece, piece, ga_s.at[n], ga_r.at[n], peer(order[0], d)[1]))
            pass_on(s, d)
        started["H", s] = halves

    def finish(s):
        if s in RELAYED:
            for copy in started["H", s]:
                copy.wait()
            pass_on(s, 2)
        else:
            for d in (1, 3, 2):
                started["A", s][d].wait()
                pass_on(s, d)

    def assemble(s):
        at, count, order = STREAMS[s]
        for copy in started["out", s]:
            copy.wait()
        for tile in range(at, at + count):
            for half in range(2):
                A, B = SLOTS[half][tile]
                pick = slice(tile * N, (tile + 1) * N)
                value = full[half, pick, :] * rden[half, pick, :]
                high, low = split(value)
                down, across = slice(A * N, (A + 1) * N), slice(B * N, (B + 1) * N)
                c_high[down, across] = high
                c_low[down, across] = low
                if A < B:
                    high, low = split(value.T)
                    c_high[across, down] = high
                    c_low[across, down] = low

    arrive(0)
    early_products()
    arrive(1)
    late_products(0)
    for copy in copies:
        copy.wait()
    table[r] = (table_y[0] + table_y[1]) + (table_y[2] + table_y[3])
    copies = [
        send(table.at[r], table.at[r], tab_s.at[5 + d], tab_r.at[5 + d], peer("z", d)[1])
        for d in range(1, 4)
    ]
    table_forward = [send(table.at[r], table.at[r], tf_s.at[0], tf_r.at[0], partner)]
    for copy in starts:
        copy.wait()
    arrive(2)
    for s in (0, 1):
        scatter_b(s)
    late_products(1)

    def table_pass(_):
        for d, copy in zip(range(1, 4), copies):
            copy.wait()
            source = ((place["z"] - d + 4) % 4) * 2 + core
            table_forward.append(send(table.at[source], table.at[source], tf_s.at[d], tf_r.at[d], partner))

    def table_done(_):
        for copy in table_forward:
            copy.wait()
        for source in range(8):
            for side in range(2):
                high, low = split(table[source, side * PART : (side + 1) * PART, :])
                at = side * HALF + source * PART
                lookup_in[at : at + PART, 0:N] = high
                lookup_in[at : at + PART, N:] = low

    def norms(item):
        half, J = item
        odd = (half + J) % 2
        right = slice(J * 2 * N, (J + 1) * 2 * N)
        picks = [tile_at(2 * i + odd) for i in range(J + 1)]
        sums_in = jnp.concatenate([lookup_in[pick, :] for pick in picks], axis=0)
        select = jnp.concatenate([lookup[pick, :] for pick in picks], axis=0)
        value = lax.rsqrt(nt(sums_in, lookup[right, :]) * nt(select, lookup_in[right, :]) + EPS)
        for i in range(J + 1):
            for k in range(2):
                tile = (2 * i + odd, 2 * J + k)
                if tile in PLACE[half]:
                    at = PLACE[half][tile]
                    rden[half, tile_at(at), :] = value[i * N : (i + 1) * N, k * N : (k + 1) * N]

    tasks = [(3.2, table_pass, 0), (4.6, table_done, 0)]
    for n, J in enumerate((2, 1, 0, 5, 4, 3)):
        tasks += [(5.3 + n, norms, (0, J)), (5.8 + n, norms, (1, J))]
    for s, start_at in zip((0, 1), (0.0, 0.1)):
        tasks += [(1.7 + start_at, spread_c, s), (6.2 + start_at, gather_b, s), (11.5 + start_at, gather_a, s)]
        if s in RELAYED:
            tasks += [(19.0 + start_at, relay, s)]
        tasks += [(21.8 + start_at, finish, s), (22.2 + start_at, assemble, s)]
    for n, s in enumerate(HELD_BACK):
        tasks.append((1.9 + n * 0.01, scatter_a, s))
    for s in range(2, len(STREAMS)):
        chunk = (s - 2) // 3
        start_at = 2.2 * chunk + 0.01 * s + (0.8 if s in HELD_BACK else 0.0)
        tasks += [(3.5 + start_at, scatter_b, s), (7.4 + start_at, spread_c, s)]
        tasks += [(11.3 + start_at, gather_b, s)]
        start_at = 2.2 * chunk + 0.01 * s
        if s in RELAYED:
            tasks += [(17.2 + start_at, gather_a, s), (21.0 + start_at, relay, s)]
            tasks += [(25.8 + start_at, finish, s), (26.0 + start_at, assemble, s)]
        else:
            tasks += [(19.6 + start_at, gather_a, s), (26 + start_at, finish, s), (26.5 + start_at, assemble, s)]
    for start_at, task, s in sorted(tasks, key=lambda item: item[0]):
        task(s)

    def times_matrix(high, low):
        wide = nn(jnp.concatenate([high, low], axis=0), c_high[...])
        return wide[0:32] + wide[32:64] + nn(high, c_low[...])

    def gram_of(high, low):
        return nt(high, high) + (nt(high, low) + nt(low, high))

    def solved(inverse, high, low):
        inverse_high, inverse_low = split(inverse)
        return nn(inverse_high, high) + (nn(inverse_high, low) + nn(inverse_low, high))

    wt[...] = first[...].T[0:32, :]

    def iterate(step, carry):
        high, low = split(times_matrix(*split(wt[...])))
        inverse = lower_inverse(gram_of(high, low))
        wt[...] = solved(inverse, high, low)
        return carry

    lax.fori_loop(0, ITERS, iterate, 0)
    first[:, 0:32] = (wt[...] * math.sqrt(1536)).T
    basis_out[...] = first[rows_at(here, PART), :].T[0:32, :]
    lane = jnp.minimum(here // N, 1536 // N - 2) * N
    window = pl.ds(pl.multiple_of(lane, N), 2 * N)
    shift = (2 * N - (here - lane)) % (2 * N)
    for side in range(2):
        pick = pl.ds(pl.multiple_of(side * HALF + r * PART, 16), PART)
        block = c_high[pick, window].astype(F32) + c_low[pick, window].astype(F32)
        block_out[side * PART : (side + 1) * PART, :] = pltpu.roll(block, shift, 1)[:, 0:PART]


def local(coefs, tilts, start_basis):
    vmem = pl.BlockSpec(memory_space=pltpu.VMEM)
    dma = pltpu.SemaphoreType.DMA
    block, basis = pl.pallas_call(
        kernel,
        out_shape=(
            pltpu.VMEM((ROWS, PART), F32),
            pltpu.VMEM((32, PART), F32),
        ),
        in_specs=[pl.BlockSpec(memory_space=pltpu.HBM)] * 3,
        out_specs=(vmem, vmem),
        scratch_shapes=[
            pltpu.VMEM((2, 1536), jnp.int32),
            pltpu.VMEM((32, PART), F32),
            pltpu.VMEM((2, ROWS, 1024), F32),
            pltpu.VMEM((8, 2, ROWS, N), F32),
            pltpu.VMEM((8, 2, ROWS, N), F32),
            pltpu.VMEM((2, 1536, 2 * N), BF16),
            pltpu.VMEM((2, 1536, 2 * N), BF16),
            pltpu.VMEM((1536, 2 * N), F32),
            pltpu.VMEM((1536, N), F32),
            pltpu.VMEM((N, N), F32),
            pltpu.VMEM((TILES * N, N), F32),
            pltpu.VMEM((11, 3, MOST * 32, N), F32),
            pltpu.VMEM((11, 3, MOST * 8, N), F32),
            pltpu.VMEM((11, 4, MOST * 8, N), F32),
            pltpu.VMEM((11, MOST * 32, N), F32),
            pltpu.VMEM((2, TILES * N, N), F32),
            pltpu.VMEM((2, TILES * N, N), F32),
            pltpu.VMEM((4, ROWS, N), F32),
            pltpu.VMEM((4, ROWS, N), F32),
            pltpu.VMEM((8, ROWS, N), F32),
            pltpu.VMEM((1536, 2 * N), BF16),
            pltpu.VMEM((1536, 2 * N), BF16),
            pltpu.VMEM((1536, N), F32),
            pltpu.VMEM((1536, 1536), BF16),
            pltpu.VMEM((1536, 1536), BF16),
            pltpu.VMEM((32, 1536), F32),
            dma((3,)),
            dma((21,)), dma((21,)), dma((24,)), dma((24,)),
            dma((9,)), dma((9,)), dma((4,)), dma((4,)), dma((9,)), dma((9,)),
            dma((33,)), dma((33,)), dma((33,)), dma((33,)), dma((33,)), dma((33,)),
            dma((33,)), dma((33,)), dma((44,)), dma((44,)), dma((44,)), dma((44,)),
        ],
        compiler_params=pltpu.CompilerParams(
            collective_id=0, has_side_effects=True, vmem_limit_bytes=55296 << 10
        ),
        name="whole",
    )(coefs, tilts.T, start_basis.T)
    return block, basis.T


def solution(mesh):
    in_specs = (P(None, "row", "col"), P(), P("col", None))
    out_specs = (P("row", "col"), P("col", None))
    return jax.shard_map(local, mesh=mesh, in_specs=in_specs, out_specs=out_specs, check_vma=False)
```

```python
import math

import jax
import jax.numpy as jnp
from jax import lax
from jax.experimental import pallas as pl
from jax.experimental.pallas import tpu as pltpu
from jax.sharding import PartitionSpec as P

GRID = 32
ITERS = 4
EPS = 1e-06
MESH = pl.DeviceIdType.MESH
F32 = jnp.float32
BF16 = jnp.bfloat16
F8 = jnp.float8_e4m3fn

ROWS = 192
PART = 96
N = 128
LOW = 8
WIDE = 6

HALF = 768

SLOTS = ([], [])
for wave in ((2, 1, 0), (5, 4, 3)):
    for J in wave:
        for half in range(2):
            odd = (half + J) % 2
            SLOTS[half].extend((2 * i + odd, 2 * J + k) for i in range(J) for k in range(2))
            SLOTS[half].append((2 * J + odd, 2 * J + 1))
        if J in (0, 4, 3):
            low = J - J % 2
            SLOTS[0].append((2 * low, 2 * low))
            SLOTS[1].append((2 * low + 2, 2 * low + 2))
PLACE = [{tile: n for n, tile in enumerate(slots)} for slots in SLOTS]
TILES = len(SLOTS[0])
ORDERS = (("x", "y", "z"), ("y", "x", "z"), ("z", "x", "y"))
STREAMS = [(0, 5, ("x", "y", "z")), (5, 5, ("y", "x", "z"))]
for counts in ((4, 3, 3), (3, 4, 3), (3, 3, 3)):
    for count, order in zip(counts, ORDERS):
        STREAMS.append((STREAMS[-1][0] + STREAMS[-1][1], count, order))
MOST = 5
RELAYED = (0, 1)
HELD_BACK = (7, 10)
PANEL = 16


def nt(left, right):
    return lax.dot_general(left, right, (((1,), (1,)), ((), ())), preferred_element_type=F32)


def nn(left, right):
    return lax.dot_general(left, right, (((1,), (0,)), ((), ())), preferred_element_type=F32)


def split(value):
    high = value.astype(BF16)
    return high, (value - high.astype(F32)).astype(BF16)


def rows_at(at, size):
    return pl.ds(pl.multiple_of(at, 8), size)


def lower_inverse(gram):
    row_of = lax.broadcasted_iota(jnp.int32, (32, 32), 0)
    column_of = lax.broadcasted_iota(jnp.int32, (32, 32), 1)

    def everywhere(value):
        return jnp.broadcast_to(value, (32, 32))

    inverse = jnp.where(row_of == column_of, 1.0, 0.0).astype(F32)
    pivots = jnp.ones((32, 32), F32)
    for j in range(0, 32, PANEL):
        columns = [everywhere(gram[:, j + q : j + q + 1]) for q in range(PANEL)]
        for p in range(PANEL):
            at = slice(j + p, j + p + 1)
            pivot = everywhere(columns[p][at, :])
            pivots = jnp.where(row_of == j + p, pivot, pivots)
            factor = jnp.where(row_of > j + p, columns[p] * (1.0 / pivot), 0.0)
            for q in range(p + 1, PANEL):
                columns[q] = columns[q] - factor * everywhere(columns[q][at, :])
            gram = gram - factor * everywhere(gram[at, :])
            inverse = inverse - factor * everywhere(inverse[at, :])
    return inverse * lax.rsqrt(pivots)


def kernel(
    coefs, tilts_in, start_in,
    block_out, basis_out,
    tilts, start, held, own, other, x_high, x_low, masks, chosen, corner,
    partial, recv_a, recv_b, recv_c, acc, full, rden,
    table_x, table_y, table, lookup, lookup_in, first,
    c_high, c_low, grow, wt,
    held_s, a2a_s, a2a_r, fwd_s, fwd_r, tab_s, tab_r, tf_s, tf_r, st_s, st_r,
    ra_s, ra_r, rb_s, rb_r, rc_s, rc_r, gb_s, gb_r, ga_s, ga_r, out_s, out_r,
):
    r = lax.axis_index("row")
    c = lax.axis_index("col")
    core = r % 2
    mate = r + 1 - 2 * core
    place = {"x": c % 4, "y": c // 4, "z": r // 2}

    def peer(axis, d):
        p = (place[axis] + d) % 4
        if axis == "x":
            return p, (r, place["y"] * 4 + p)
        if axis == "y":
            return p, (r, p * 4 + place["x"])
        return p, (p * 2 + core, c)

    partner = (mate, c)

    def send(src, dst, ss, rs, device):
        copy = pltpu.make_async_remote_copy(
            src_ref=src, dst_ref=dst, send_sem=ss, recv_sem=rs,
            device_id=device, device_id_type=MESH,
        )
        copy.start()
        return copy

    barrier = pltpu.get_barrier_semaphore()
    for d in range(1, 8):
        pl.semaphore_signal(barrier, inc=1, device_id=((r + d) % 8, c), device_id_type=MESH)
    for axis in ("x", "y"):
        for d in range(1, 4):
            pl.semaphore_signal(barrier, inc=1, device_id=peer(axis, d)[1], device_id_type=MESH)
    held_copy = pltpu.make_async_copy(coefs, held, held_s.at[0])
    held_copy.start()
    small_copies = [
        pltpu.make_async_copy(start_in, start, held_s.at[1]),
        pltpu.make_async_copy(tilts_in, tilts, held_s.at[2]),
    ]
    for copy in small_copies:
        copy.start()
    mine = pl.ds(pl.multiple_of(r * N, N), N)
    corner[...] = jnp.zeros((N, N), F32)
    small_copies[0].wait()
    corner[0:32, 0:PART] = start[...]
    here = (c % 2 * 8 + c // 2) * PART
    first[rows_at(here, PART), :] = corner[...].T[0:PART, :]
    held_copy.wait()
    pl.semaphore_wait(barrier, 13)

    cuts = (
        (slice(0, 2), pl.ds(0, PART)),
        (slice(0, 1), pl.ds(PART, PART)),
        (slice(1, 2), pl.ds(PART, PART)),
    )
    exchange = ([], [], [])
    forward = ([], [], [])
    for step, (parts, rows) in enumerate(cuts):
        for n, d in enumerate((2, 6, 1, 7, 3, 5, 4)):
            p = (r + d) % 8
            n = 7 * step + n
            exchange[step].append((d, send(
                held.at[parts, rows, pl.ds(pl.multiple_of(p * N, N), N)],
                own.at[r, parts, rows], a2a_s.at[n], a2a_r.at[n], (p, c),
            )))
        forward[step].append(send(
            held.at[parts, rows, mine], other.at[r, parts, rows],
            fwd_s.at[8 * step], fwd_r.at[8 * step], partner,
        ))
    own_rows = rows_at(here, PART)
    starts = [
        send(first.at[own_rows], first.at[own_rows], st_s.at[d - 1], st_r.at[d - 1], peer("x", d)[1])
        for d in range(1, 4)
    ]

    small_copies[1].wait()
    low_side = tilts[0:1, :]
    high_side = tilts[1:2, :]
    line = lax.broadcasted_iota(jnp.int32, (N, 1536), 0)
    picked = (line == high_side - LOW) | (line == low_side - LOW + 64)
    picked = jnp.where(picked, 1.0, 0.0)
    picked = jnp.where(line == 126, low_side.astype(F32), picked)
    picked = jnp.where(line == 127, high_side.astype(F32), picked)
    picked = picked.T
    for n in range(16):
        at = (n % 2 * 8 + n // 2) * PART
        chosen[at : at + PART, :] = picked[n * PART : (n + 1) * PART, :]
    column = lax.broadcasted_iota(jnp.int32, (1536, N), 1)
    one_hot = jnp.where(column < 126, chosen[...], 0.0).astype(BF16)
    lookup[:, 0:N] = one_hot
    lookup[:, N:] = one_hot

    def waves(at, count):
        wave = at + lax.broadcasted_iota(jnp.int32, (1, count), 1)
        wave_x = jnp.abs(wave // (GRID * (GRID // 2)) - GRID // 2).astype(F32)
        wave_z = wave % GRID - GRID // 2
        return wave_x, wave_z >= 0, (jnp.abs(wave_z) * 16).astype(F32)

    def wedge(pick, wave):
        wave_x, upward, need = wave
        limit = jnp.where(upward, chosen[pick, 127:128], chosen[pick, 126:127])
        return jnp.where(need <= limit * wave_x, 1.0, 0.0)

    for side, position in enumerate((r, mate)):
        wave = waves(c * 1024 + position * N, N)
        for source in range(8):
            pick = pl.ds(source * ROWS, ROWS)
            masks[pick, side * N : (side + 1) * N] = wedge(pick, wave)

    own[r] = held[:, :, mine]

    wave = waves(c * 1024, 1024)
    wave_x, upward, need = wave
    own_mask = jnp.concatenate(
        [wedge(rows_at(r * PART, PART), wave), wedge(rows_at(HALF + r * PART, PART), wave)], axis=0
    )
    real, imag = held[0] * own_mask, held[1] * own_mask
    energy = real * real + imag * imag
    slope = lax.broadcasted_iota(jnp.int32, (N, 1), 0)
    below = need <= (slope % 64 + LOW).astype(F32) * wave_x
    side = jnp.where(slope < 64, 1, 0) == jnp.where(upward, 1, 0)
    pattern = jnp.where(below & side, 1.0, 0.0).astype(BF16)
    high = energy.astype(BF16)
    middle, low = split(energy - high.astype(F32))
    sums = nt(high, pattern) + nt(middle, pattern) + nt(low, pattern)

    def ring_send(buffer, value, axis, base):
        buffer[place[axis]] = value
        return [
            send(
                buffer.at[place[axis]], buffer.at[place[axis]],
                tab_s.at[base + d - 1], tab_r.at[base + d - 1], peer(axis, d)[1],
            )
            for d in range(1, 4)
        ]

    copies = ring_send(table_x, sums, "x", 0)
    for copy in starts:
        copy.wait()
    starts = []
    for side in range(2):
        own_rows = rows_at(side * HALF + place["y"] * 2 * PART, 2 * PART)
        for d in range(1, 4):
            n = 3 * side + d + 2
            starts.append(send(first.at[own_rows], first.at[own_rows], st_s.at[n], st_r.at[n], peer("y", d)[1]))
    for copy in copies:
        copy.wait()
    copies = ring_send(table_y, (table_x[0] + table_x[1]) + (table_x[2] + table_x[3]), "y", 3)

    def arrive(step):
        parts, rows = cuts[step]
        for n, (d, copy) in enumerate(exchange[step]):
            copy.wait()
            source = (r - d + 8) % 8
            n = 8 * step + n + 1
            forward[step].append(send(
                own.at[source, parts, rows], other.at[source, parts, rows], fwd_s.at[n], fwd_r.at[n], partner,
            ))
        base = 0 if step == 0 else HALF
        for side, ref in enumerate((own, other)):
            if side == 1:
                for copy in forward[step]:
                    copy.wait()
            lane = slice(side * N, (side + 1) * N)
            for source in range(8):
                pick = pl.ds(base + source * PART, PART)
                mask = masks[pick, lane]
                for part in range(parts.start, parts.stop):
                    high, low = split(ref[source, part, rows, :] * mask)
                    x_high[part, pick, lane] = high
                    x_low[part, pick, lane] = low

    started = {}

    def scatter(s, source, buffer, size, axis, ss, rs):
        copies = []
        for d in range(1, 4):
            p, device = peer(axis, d)
            n = 3 * s + d - 1
            copies.append(send(
                source.at[rows_at(p * size, size)],
                buffer.at[s, d - 1, pl.ds(0, size)], ss.at[n], rs.at[n], device,
            ))
        return copies

    def scatter_a(s):
        at, count, order = STREAMS[s]
        source = partial.at[pl.ds(at * N, count * N)]
        started["a", s] = scatter(s, source, recv_a, count * 32, order[0], ra_s, ra_r)

    def product(J, part):
        odd = (core + J) % 2
        right_high = x_high[part, J * 2 * N : (J + 1) * 2 * N, :]
        right_low = x_low[part, J * 2 * N : (J + 1) * 2 * N, :]
        picks = [pl.ds(pl.multiple_of((2 * i + odd) * N, N), N) for i in range(J + 1)]
        left_high = jnp.concatenate([x_high[part, pick, :] for pick in picks], axis=0)
        left_low = jnp.concatenate([x_low[part, pick, :] for pick in picks], axis=0)
        return nt(left_high, right_high) + nt(left_high, right_low) + nt(left_low, right_high)

    def cut(J, value):
        tiles = [value[i * N : (i + 1) * N, k * N : (k + 1) * N] for i in range(J + 1) for k in range(2)]
        return tiles.pop(2 * J), tiles

    def tile_at(n):
        return slice(n * N, (n + 1) * N)

    def early_products():
        at = 0
        spares = {}
        for J in (2, 1, 0):
            spares[J], tiles = cut(J, product(J, 0) + product(J, 1))
            if J == 0:
                tiles.append(jnp.where(core == 0, spares[0], spares[1]))
            for tile in tiles:
                partial[tile_at(at), :] = tile
                at += 1
        corner[...] = spares[2]
        for s in (0, 1):
            scatter_a(s)

    def late_products(part):
        at = 10
        stream = 2
        spares = {}
        for J in (5, 4, 3):
            spares[J], tiles = cut(J, product(J, part))
            if J == 4:
                tiles.append(jnp.where(core == 0, spares[4], spares[5]))
            if J == 3:
                kept = corner[...] if part == 0 else jnp.zeros((N, N), F32)
                tiles.append(jnp.where(core == 0, kept, spares[3]))
            for tile in tiles:
                if part == 0:
                    partial[tile_at(at), :] = tile
                else:
                    partial[tile_at(at), :] += tile
                at += 1
            while part == 1 and stream < len(STREAMS) and sum(STREAMS[stream][:2]) <= at:
                if stream not in HELD_BACK:
                    scatter_a(stream)
                stream += 1

    def scatter_b(s):
        count, order = STREAMS[s][1:]
        size = count * 32
        for copy in started["a", s]:
            copy.wait()
        pick = rows_at(STREAMS[s][0] * N + place[order[0]] * size, size)
        got = [recv_a[s, n, 0:size, :] for n in range(3)]
        acc[s, 0:size, :] = (partial[pick, :] + got[0]) + (got[1] + got[2])
        started["b", s] = scatter(s, acc.at[s], recv_b, count * 8, order[1], rb_s, rb_r)

    def spread_c(s):
        count, order = STREAMS[s][1:]
        size = count * 8
        for copy in started["b", s]:
            copy.wait()
        got = [recv_b[s, n, 0:size, :] for n in range(3)]
        value = (acc[s, rows_at(place[order[1]] * size, size), :] + got[0]) + (got[1] + got[2])
        here = place[order[2]]
        recv_c[s, here, 0:size, :] = value
        piece = recv_c.at[s, here, pl.ds(0, size)]
        started["c", s] = [
            send(piece, piece, rc_s.at[3 * s + d - 1], rc_r.at[3 * s + d - 1], peer(order[2], d)[1])
            for d in range(1, 4)
        ]

    def gather_b(s):
        at, count, order = STREAMS[s]
        size = count * 8
        for copy in started["c", s]:
            copy.wait()
        got = [recv_c[s, n, 0:size, :] for n in range(4)]
        pick = rows_at(at * N + (place[order[0]] * 4 + place[order[1]]) * size, size)
        full[core, pick, :] = (got[0] + got[1]) + (got[2] + got[3])
        piece = full.at[core, pick]
        started["B", s] = [
            send(piece, piece, gb_s.at[3 * s + d - 1], gb_r.at[3 * s + d - 1], peer(order[1], d)[1])
            for d in range(1, 4)
        ]

    def piece_of(s, d, low, size):
        at, count, order = STREAMS[s]
        seg = (place[order[0]] - d + 4) % 4 * count * 32
        return full.at[core, rows_at(at * N + seg + low, size)]

    def gather_a(s):
        count, order = STREAMS[s][1:]
        for copy in started["B", s]:
            copy.wait()
        piece = piece_of(s, 0, 0, count * 32)
        started["A", s] = {
            d: send(piece, piece, ga_s.at[3 * s + d - 1], ga_r.at[3 * s + d - 1], peer(order[0], d)[1])
            for d in ((1, 3) if s in RELAYED else (1, 3, 2))
        }
        started["out", s] = []
        pass_on(s, 0)

    def pass_on(s, d):
        piece = piece_of(s, d, 0, STREAMS[s][1] * 32)
        started["out", s].append(send(piece, piece, out_s.at[4 * s + d], out_r.at[4 * s + d], partner))

    def relay(s):
        count, order = STREAMS[s][1:]
        halves = []
        for d, low in ((1, 0), (3, count * 16)):
            started["A", s][d].wait()
            piece = piece_of(s, d, low, count * 16)
            n = 3 * s + 1 if d == 1 else 33 + s
            halves.append(send(piece, piece, ga_s.at[n], ga_r.at[n], peer(order[0], d)[1]))
            pass_on(s, d)
        started["H", s] = halves

    def finish(s):
        if s in RELAYED:
            for copy in started["H", s]:
                copy.wait()
            pass_on(s, 2)
        else:
            for d in (1, 3, 2):
                started["A", s][d].wait()
                pass_on(s, d)

    def assemble(s):
        at, count, order = STREAMS[s]
        for copy in started["out", s]:
            copy.wait()
        for tile in range(at, at + count):
            for half in range(2):
                A, B = SLOTS[half][tile]
                pick = slice(tile * N, (tile + 1) * N)
                value = full[half, pick, :] * rden[half, pick, :]
                high = value.astype(BF16)
                low = (value - high.astype(F32)) * grow[0:1, :]
                down, across = slice(A * N, (A + 1) * N), slice(B * N, (B + 1) * N)
                c_high[down, across] = high
                c_low[down, across] = low.astype(F8)
                if A < B:
                    c_high[across, down] = value.T.astype(BF16)
                    c_low[across, down] = low.T.astype(F8)

    arrive(0)
    early_products()
    arrive(1)
    late_products(0)
    for copy in copies:
        copy.wait()
    table[r] = (table_y[0] + table_y[1]) + (table_y[2] + table_y[3])
    copies = [
        send(table.at[r], table.at[r], tab_s.at[5 + d], tab_r.at[5 + d], peer("z", d)[1])
        for d in range(1, 4)
    ]
    table_forward = [send(table.at[r], table.at[r], tf_s.at[0], tf_r.at[0], partner)]
    for copy in starts:
        copy.wait()
    arrive(2)
    for s in (0, 1):
        scatter_b(s)
    late_products(1)

    def table_pass(_):
        for d, copy in zip(range(1, 4), copies):
            copy.wait()
            source = ((place["z"] - d + 4) % 4) * 2 + core
            table_forward.append(send(table.at[source], table.at[source], tf_s.at[d], tf_r.at[d], partner))

    def table_done(_):
        for copy in table_forward:
            copy.wait()
        for source in range(8):
            for side in range(2):
                high, low = split(table[source, side * PART : (side + 1) * PART, :])
                at = side * HALF + source * PART
                lookup_in[at : at + PART, 0:N] = high
                lookup_in[at : at + PART, N:] = low
        most = jnp.max(jnp.max(table[...], axis=0), axis=0, keepdims=True)
        most = 2.0 * jnp.max(most, axis=1, keepdims=True)
        factor = 65536.0 * jnp.sqrt(most * most + EPS) / jnp.maximum(most, 1e-30)
        grow[...] = jnp.broadcast_to(factor, (8, N))

    def norms(item):
        half, J = item
        odd = (half + J) % 2
        right = slice(J * 2 * N, (J + 1) * 2 * N)
        picks = [tile_at(2 * i + odd) for i in range(J + 1)]
        sums_in = jnp.concatenate([lookup_in[pick, :] for pick in picks], axis=0)
        select = jnp.concatenate([lookup[pick, :] for pick in picks], axis=0)
        value = lax.rsqrt(nt(sums_in, lookup[right, :]) * nt(select, lookup_in[right, :]) + EPS)
        for i in range(J + 1):
            for k in range(2):
                tile = (2 * i + odd, 2 * J + k)
                if tile in PLACE[half]:
                    at = PLACE[half][tile]
                    rden[half, tile_at(at), :] = value[i * N : (i + 1) * N, k * N : (k + 1) * N]

    tasks = [(3.2, table_pass, 0), (4.6, table_done, 0)]
    for n, J in enumerate((2, 1, 0, 5, 4, 3)):
        tasks += [(5.3 + n, norms, (0, J)), (5.8 + n, norms, (1, J))]
    for s, start_at in zip((0, 1), (0.0, 0.1)):
        tasks += [(1.7 + start_at, spread_c, s), (6.2 + start_at, gather_b, s), (11.5 + start_at, gather_a, s)]
        if s in RELAYED:
            tasks += [(19.0 + start_at, relay, s)]
        tasks += [(21.8 + start_at, finish, s), (22.2 + start_at, assemble, s)]
    for n, s in enumerate(HELD_BACK):
        tasks.append((1.9 + n * 0.01, scatter_a, s))
    for s in range(2, len(STREAMS)):
        chunk = (s - 2) // 3
        start_at = 2.2 * chunk + 0.01 * s + (0.8 if s in HELD_BACK else 0.0)
        tasks += [(3.5 + start_at, scatter_b, s), (7.4 + start_at, spread_c, s)]
        tasks += [(11.3 + start_at, gather_b, s)]
        start_at = 2.2 * chunk + 0.01 * s
        if s in RELAYED:
            tasks += [(17.2 + start_at, gather_a, s), (21.0 + start_at, relay, s)]
            tasks += [(25.8 + start_at, finish, s), (26.0 + start_at, assemble, s)]
        else:
            tasks += [(19.6 + start_at, gather_a, s), (26 + start_at, finish, s), (26.5 + start_at, assemble, s)]
    for start_at, task, s in sorted(tasks, key=lambda item: item[0]):
        task(s)

    def times_matrix(high, low):
        wide = nn(jnp.concatenate([high, low], axis=0), c_high[...])
        return wide[0:32] + (wide[32:64] + nn(high, c_low[...]) * (1.0 / grow[0:1, 0:1]))

    def gram_of(high, low):
        return nt(high, high) + (nt(high, low) + nt(low, high))

    def solved(inverse, high, low):
        inverse_high, inverse_low = split(inverse)
        return nn(inverse_high, high) + (nn(inverse_high, low) + nn(inverse_low, high))

    wt[...] = first[...].T[0:32, :]

    def iterate(step, carry):
        high, low = split(times_matrix(*split(wt[...])))
        inverse = lower_inverse(gram_of(high, low))
        wt[...] = solved(inverse, high, low)
        return carry

    lax.fori_loop(0, ITERS, iterate, 0)
    first[:, 0:32] = (wt[...] * math.sqrt(1536)).T
    basis_out[...] = first[rows_at(here, PART), :].T[0:32, :]
    lane = jnp.minimum(here // N, 1536 // N - 2) * N
    window = pl.ds(pl.multiple_of(lane, N), 2 * N)
    shift = (2 * N - (here - lane)) % (2 * N)
    for side in range(2):
        pick = pl.ds(pl.multiple_of(side * HALF + r * PART, 32), PART)
        block = c_high[pick, window].astype(F32) + c_low[pick, window].astype(F32) * (1.0 / grow[0:1, 0:1])
        block_out[side * PART : (side + 1) * PART, :] = pltpu.roll(block, shift, 1)[:, 0:PART]


def local(coefs, tilts, start_basis):
    vmem = pl.BlockSpec(memory_space=pltpu.VMEM)
    dma = pltpu.SemaphoreType.DMA
    block, basis = pl.pallas_call(
        kernel,
        out_shape=(
            pltpu.VMEM((ROWS, PART), F32),
            pltpu.VMEM((32, PART), F32),
        ),
        in_specs=[pl.BlockSpec(memory_space=pltpu.HBM)] * 3,
        out_specs=(vmem, vmem),
        scratch_shapes=[
            pltpu.VMEM((2, 1536), jnp.int32),
            pltpu.VMEM((32, PART), F32),
            pltpu.VMEM((2, ROWS, 1024), F32),
            pltpu.VMEM((8, 2, ROWS, N), F32),
            pltpu.VMEM((8, 2, ROWS, N), F32),
            pltpu.VMEM((2, 1536, 2 * N), BF16),
            pltpu.VMEM((2, 1536, 2 * N), BF16),
            pltpu.VMEM((1536, 2 * N), F32),
            pltpu.VMEM((1536, N), F32),
            pltpu.VMEM((N, N), F32),
            pltpu.VMEM((TILES * N, N), F32),
            pltpu.VMEM((11, 3, MOST * 32, N), F32),
            pltpu.VMEM((11, 3, MOST * 8, N), F32),
            pltpu.VMEM((11, 4, MOST * 8, N), F32),
            pltpu.VMEM((11, MOST * 32, N), F32),
            pltpu.VMEM((2, TILES * N, N), F32),
            pltpu.VMEM((2, TILES * N, N), F32),
            pltpu.VMEM((4, ROWS, N), F32),
            pltpu.VMEM((4, ROWS, N), F32),
            pltpu.VMEM((8, ROWS, N), F32),
            pltpu.VMEM((1536, 2 * N), BF16),
            pltpu.VMEM((1536, 2 * N), BF16),
            pltpu.VMEM((1536, N), F32),
            pltpu.VMEM((1536, 1536), BF16),
            pltpu.VMEM((1536, 1536), F8),
            pltpu.VMEM((8, N), F32),
            pltpu.VMEM((32, 1536), F32),
            dma((3,)),
            dma((21,)), dma((21,)), dma((24,)), dma((24,)),
            dma((9,)), dma((9,)), dma((4,)), dma((4,)), dma((9,)), dma((9,)),
            dma((33,)), dma((33,)), dma((33,)), dma((33,)), dma((33,)), dma((33,)),
            dma((33,)), dma((33,)), dma((44,)), dma((44,)), dma((44,)), dma((44,)),
        ],
        compiler_params=pltpu.CompilerParams(
            collective_id=0, has_side_effects=True, vmem_limit_bytes=55296 << 10
        ),
        name="whole",
    )(coefs, tilts.T, start_basis.T)
    return block, basis.T


def solution(mesh):
    in_specs = (P(None, "row", "col"), P(), P("col", None))
    out_specs = (P("row", "col"), P("col", None))
    return jax.shard_map(local, mesh=mesh, in_specs=in_specs, out_specs=out_specs, check_vma=False)
```

```python
import math

import jax
import jax.numpy as jnp
from jax import lax
from jax.experimental import pallas as pl
from jax.experimental.pallas import tpu as pltpu
from jax.sharding import PartitionSpec as P

GRID = 32
ITERS = 4
EPS = 1e-06
MESH = pl.DeviceIdType.MESH
F32 = jnp.float32
BF16 = jnp.bfloat16
F8 = jnp.float8_e4m3fn

ROWS = 192
PART = 96
N = 128
LOW = 8
WIDE = 6

HALF = 768

SLOTS = ([], [])
for wave in ((2, 1, 0), (5, 4, 3)):
    for J in wave:
        for half in range(2):
            odd = (half + J) % 2
            SLOTS[half].extend((2 * i + odd, 2 * J + k) for i in range(J) for k in range(2))
            SLOTS[half].append((2 * J + odd, 2 * J + 1))
        if J in (0, 4, 3):
            low = J - J % 2
            SLOTS[0].append((2 * low, 2 * low))
            SLOTS[1].append((2 * low + 2, 2 * low + 2))
PLACE = [{tile: n for n, tile in enumerate(slots)} for slots in SLOTS]
TILES = len(SLOTS[0])
ORDERS = (("x", "y", "z"), ("y", "x", "z"), ("z", "x", "y"))
STREAMS = [(0, 5, ("x", "y", "z")), (5, 5, ("y", "x", "z"))]
for counts in ((4, 3, 3), (3, 4, 3), (3, 3, 3)):
    for count, order in zip(counts, ORDERS):
        STREAMS.append((STREAMS[-1][0] + STREAMS[-1][1], count, order))
MOST = 5
RELAYED = (0, 1)
HELD_BACK = (7, 10)
PANEL = 16


def nt(left, right):
    return lax.dot_general(left, right, (((1,), (1,)), ((), ())), preferred_element_type=F32)


def nn(left, right):
    return lax.dot_general(left, right, (((1,), (0,)), ((), ())), preferred_element_type=F32)


def split(value):
    high = value.astype(BF16)
    return high, (value - high.astype(F32)).astype(BF16)


def rows_at(at, size):
    return pl.ds(pl.multiple_of(at, 8), size)


def lower_inverse(gram):
    row_of = lax.broadcasted_iota(jnp.int32, (32, 32), 0)
    column_of = lax.broadcasted_iota(jnp.int32, (32, 32), 1)

    def everywhere(value):
        return jnp.broadcast_to(value, (32, 32))

    inverse = jnp.where(row_of == column_of, 1.0, 0.0).astype(F32)
    pivots = jnp.ones((32, 32), F32)
    for j in range(0, 32, PANEL):
        columns = [everywhere(gram[:, j + q : j + q + 1]) for q in range(PANEL)]
        for p in range(PANEL):
            at = slice(j + p, j + p + 1)
            pivot = everywhere(columns[p][at, :])
            pivots = jnp.where(row_of == j + p, pivot, pivots)
            factor = jnp.where(row_of > j + p, columns[p] * (1.0 / pivot), 0.0)
            for q in range(p + 1, PANEL):
                columns[q] = columns[q] - factor * everywhere(columns[q][at, :])
            gram = gram - factor * everywhere(gram[at, :])
            inverse = inverse - factor * everywhere(inverse[at, :])
    return inverse * lax.rsqrt(pivots)


def kernel(
    coefs, tilts_in, start_in,
    block_out, basis_out,
    tilts, start, held, own, other, x_high, x_low, masks, chosen, corner,
    partial, recv_a, recv_b, recv_c, acc, full, rden,
    table_x, table_y, table, lookup, lookup_in, first,
    c_high, c_low, grow, wt,
    held_s, a2a_s, a2a_r, fwd_s, fwd_r, tab_s, tab_r, tf_s, tf_r, st_s, st_r,
    ra_s, ra_r, rb_s, rb_r, rc_s, rc_r, gb_s, gb_r, ga_s, ga_r, out_s, out_r,
):
    r = lax.axis_index("row")
    c = lax.axis_index("col")
    core = r % 2
    mate = r + 1 - 2 * core
    place = {"x": c % 4, "y": c // 4, "z": r // 2}

    def peer(axis, d):
        p = (place[axis] + d) % 4
        if axis == "x":
            return p, (r, place["y"] * 4 + p)
        if axis == "y":
            return p, (r, p * 4 + place["x"])
        return p, (p * 2 + core, c)

    partner = (mate, c)

    def send(src, dst, ss, rs, device):
        copy = pltpu.make_async_remote_copy(
            src_ref=src, dst_ref=dst, send_sem=ss, recv_sem=rs,
            device_id=device, device_id_type=MESH,
        )
        copy.start()
        return copy

    barrier = pltpu.get_barrier_semaphore()
    for d in range(1, 8):
        pl.semaphore_signal(barrier, inc=1, device_id=((r + d) % 8, c), device_id_type=MESH)
    for axis in ("x", "y"):
        for d in range(1, 4):
            pl.semaphore_signal(barrier, inc=1, device_id=peer(axis, d)[1], device_id_type=MESH)
    held_copy = pltpu.make_async_copy(coefs, held, held_s.at[0])
    held_copy.start()
    small_copies = [
        pltpu.make_async_copy(start_in, start, held_s.at[1]),
        pltpu.make_async_copy(tilts_in, tilts, held_s.at[2]),
    ]
    for copy in small_copies:
        copy.start()
    mine = pl.ds(pl.multiple_of(r * N, N), N)
    corner[...] = jnp.zeros((N, N), F32)
    small_copies[0].wait()
    corner[0:32, 0:PART] = start[...]
    here = (c % 2 * 8 + c // 2) * PART
    first[rows_at(here, PART), :] = corner[...].T[0:PART, :]
    held_copy.wait()
    pl.semaphore_wait(barrier, 13)

    cuts = (
        (slice(0, 2), pl.ds(0, PART)),
        (slice(0, 1), pl.ds(PART, PART)),
        (slice(1, 2), pl.ds(PART, PART)),
    )
    exchange = ([], [], [])
    forward = ([], [], [])
    for step, (parts, rows) in enumerate(cuts):
        for n, d in enumerate((2, 6, 1, 7, 3, 5, 4)):
            p = (r + d) % 8
            n = 7 * step + n
            exchange[step].append((d, send(
                held.at[parts, rows, pl.ds(pl.multiple_of(p * N, N), N)],
                own.at[r, parts, rows], a2a_s.at[n], a2a_r.at[n], (p, c),
            )))
        forward[step].append(send(
            held.at[parts, rows, mine], other.at[r, parts, rows],
            fwd_s.at[8 * step], fwd_r.at[8 * step], partner,
        ))
    own_rows = rows_at(here, PART)
    starts = [
        send(first.at[own_rows], first.at[own_rows], st_s.at[d - 1], st_r.at[d - 1], peer("x", d)[1])
        for d in range(1, 4)
    ]

    small_copies[1].wait()
    low_side = tilts[0:1, :]
    high_side = tilts[1:2, :]
    line = lax.broadcasted_iota(jnp.int32, (N, 1536), 0)
    picked = (line == high_side - LOW) | (line == low_side - LOW + 64)
    picked = jnp.where(picked, 1.0, 0.0)
    picked = jnp.where(line == 126, low_side.astype(F32), picked)
    picked = jnp.where(line == 127, high_side.astype(F32), picked)
    picked = picked.T
    for n in range(16):
        at = (n % 2 * 8 + n // 2) * PART
        chosen[at : at + PART, :] = picked[n * PART : (n + 1) * PART, :]
    column = lax.broadcasted_iota(jnp.int32, (1536, N), 1)
    one_hot = jnp.where(column < 126, chosen[...], 0.0).astype(BF16)
    lookup[:, 0:N] = one_hot
    lookup[:, N:] = one_hot

    def waves(at, count):
        wave = at + lax.broadcasted_iota(jnp.int32, (1, count), 1)
        wave_x = jnp.abs(wave // (GRID * (GRID // 2)) - GRID // 2).astype(F32)
        wave_z = wave % GRID - GRID // 2
        return wave_x, wave_z >= 0, (jnp.abs(wave_z) * 16).astype(F32)

    def wedge(pick, wave):
        wave_x, upward, need = wave
        limit = jnp.where(upward, chosen[pick, 127:128], chosen[pick, 126:127])
        return jnp.where(need <= limit * wave_x, 1.0, 0.0)

    for side, position in enumerate((r, mate)):
        wave = waves(c * 1024 + position * N, N)
        for source in range(8):
            pick = pl.ds(source * ROWS, ROWS)
            masks[pick, side * N : (side + 1) * N] = wedge(pick, wave)

    own[r] = held[:, :, mine]

    wave = waves(c * 1024, 1024)
    wave_x, upward, need = wave
    own_mask = jnp.concatenate(
        [wedge(rows_at(r * PART, PART), wave), wedge(rows_at(HALF + r * PART, PART), wave)], axis=0
    )
    real, imag = held[0] * own_mask, held[1] * own_mask
    energy = real * real + imag * imag
    slope = lax.broadcasted_iota(jnp.int32, (N, 1), 0)
    below = need <= (slope % 64 + LOW).astype(F32) * wave_x
    side = jnp.where(slope < 64, 1, 0) == jnp.where(upward, 1, 0)
    pattern = jnp.where(below & side, 1.0, 0.0).astype(BF16)
    high = energy.astype(BF16)
    middle, low = split(energy - high.astype(F32))
    sums = nt(high, pattern) + nt(middle, pattern) + nt(low, pattern)

    def ring_send(buffer, value, axis, base):
        buffer[place[axis]] = value
        return [
            send(
                buffer.at[place[axis]], buffer.at[place[axis]],
                tab_s.at[base + d - 1], tab_r.at[base + d - 1], peer(axis, d)[1],
            )
            for d in range(1, 4)
        ]

    copies = ring_send(table_x, sums, "x", 0)
    for copy in starts:
        copy.wait()
    starts = []
    for side in range(2):
        own_rows = rows_at(side * HALF + place["y"] * 2 * PART, 2 * PART)
        for d in range(1, 4):
            n = 3 * side + d + 2
            starts.append(send(first.at[own_rows], first.at[own_rows], st_s.at[n], st_r.at[n], peer("y", d)[1]))
    for copy in copies:
        copy.wait()
    copies = ring_send(table_y, (table_x[0] + table_x[1]) + (table_x[2] + table_x[3]), "y", 3)

    def arrive(step):
        parts, rows = cuts[step]
        for n, (d, copy) in enumerate(exchange[step]):
            copy.wait()
            source = (r - d + 8) % 8
            n = 8 * step + n + 1
            forward[step].append(send(
                own.at[source, parts, rows], other.at[source, parts, rows], fwd_s.at[n], fwd_r.at[n], partner,
            ))
        base = 0 if step == 0 else HALF
        for side, ref in enumerate((own, other)):
            if side == 1:
                for copy in forward[step]:
                    copy.wait()
            lane = slice(side * N, (side + 1) * N)
            for source in range(8):
                pick = pl.ds(base + source * PART, PART)
                mask = masks[pick, lane]
                for part in range(parts.start, parts.stop):
                    high, low = split(ref[source, part, rows, :] * mask)
                    x_high[part, pick, lane] = high
                    x_low[part, pick, lane] = low

    started = {}

    def scatter(s, source, buffer, size, axis, ss, rs):
        copies = []
        for d in range(1, 4):
            p, device = peer(axis, d)
            n = 3 * s + d - 1
            copies.append(send(
                source.at[rows_at(p * size, size)],
                buffer.at[s, d - 1, pl.ds(0, size)], ss.at[n], rs.at[n], device,
            ))
        return copies

    def scatter_a(s):
        at, count, order = STREAMS[s]
        source = partial.at[pl.ds(at * N, count * N)]
        started["a", s] = scatter(s, source, recv_a, count * 32, order[0], ra_s, ra_r)

    def product(J, part):
        odd = (core + J) % 2
        right_high = x_high[part, J * 2 * N : (J + 1) * 2 * N, :]
        right_low = x_low[part, J * 2 * N : (J + 1) * 2 * N, :]
        picks = [pl.ds(pl.multiple_of((2 * i + odd) * N, N), N) for i in range(J + 1)]
        left_high = jnp.concatenate([x_high[part, pick, :] for pick in picks], axis=0)
        left_low = jnp.concatenate([x_low[part, pick, :] for pick in picks], axis=0)
        return nt(left_high, right_high) + nt(left_high, right_low) + nt(left_low, right_high)

    def cut(J, value):
        tiles = [value[i * N : (i + 1) * N, k * N : (k + 1) * N] for i in range(J + 1) for k in range(2)]
        return tiles.pop(2 * J), tiles

    def tile_at(n):
        return slice(n * N, (n + 1) * N)

    def early_products():
        at = 0
        spares = {}
        for J in (2, 1, 0):
            spares[J], tiles = cut(J, product(J, 0) + product(J, 1))
            if J == 0:
                tiles.append(jnp.where(core == 0, spares[0], spares[1]))
            for tile in tiles:
                partial[tile_at(at), :] = tile
                at += 1
        corner[...] = spares[2]
        for s in (0, 1):
            scatter_a(s)

    def late_products(part):
        at = 10
        stream = 2
        spares = {}
        for J in (5, 4, 3):
            spares[J], tiles = cut(J, product(J, part))
            if J == 4:
                tiles.append(jnp.where(core == 0, spares[4], spares[5]))
            if J == 3:
                kept = corner[...] if part == 0 else jnp.zeros((N, N), F32)
                tiles.append(jnp.where(core == 0, kept, spares[3]))
            for tile in tiles:
                if part == 0:
                    partial[tile_at(at), :] = tile
                else:
                    partial[tile_at(at), :] += tile
                at += 1
            while part == 1 and stream < len(STREAMS) and sum(STREAMS[stream][:2]) <= at:
                if stream not in HELD_BACK:
                    scatter_a(stream)
                stream += 1

    def scatter_b(s):
        count, order = STREAMS[s][1:]
        size = count * 32
        for copy in started["a", s]:
            copy.wait()
        pick = rows_at(STREAMS[s][0] * N + place[order[0]] * size, size)
        got = [recv_a[s, n, 0:size, :] for n in range(3)]
        acc[s, 0:size, :] = (partial[pick, :] + got[0]) + (got[1] + got[2])
        started["b", s] = scatter(s, acc.at[s], recv_b, count * 8, order[1], rb_s, rb_r)

    def spread_c(s):
        count, order = STREAMS[s][1:]
        size = count * 8
        for copy in started["b", s]:
            copy.wait()
        got = [recv_b[s, n, 0:size, :] for n in range(3)]
        value = (acc[s, rows_at(place[order[1]] * size, size), :] + got[0]) + (got[1] + got[2])
        here = place[order[2]]
        recv_c[s, here, 0:size, :] = value
        piece = recv_c.at[s, here, pl.ds(0, size)]
        started["c", s] = [
            send(piece, piece, rc_s.at[3 * s + d - 1], rc_r.at[3 * s + d - 1], peer(order[2], d)[1])
            for d in range(1, 4)
        ]

    def gather_b(s):
        at, count, order = STREAMS[s]
        size = count * 8
        for copy in started["c", s]:
            copy.wait()
        got = [recv_c[s, n, 0:size, :] for n in range(4)]
        pick = rows_at(at * N + (place[order[0]] * 4 + place[order[1]]) * size, size)
        full[core, pick, :] = (got[0] + got[1]) + (got[2] + got[3])
        piece = full.at[core, pick]
        started["B", s] = [
            send(piece, piece, gb_s.at[3 * s + d - 1], gb_r.at[3 * s + d - 1], peer(order[1], d)[1])
            for d in range(1, 4)
        ]

    def piece_of(s, d, low, size):
        at, count, order = STREAMS[s]
        seg = (place[order[0]] - d + 4) % 4 * count * 32
        return full.at[core, rows_at(at * N + seg + low, size)]

    def gather_a(s):
        count, order = STREAMS[s][1:]
        for copy in started["B", s]:
            copy.wait()
        piece = piece_of(s, 0, 0, count * 32)
        started["A", s] = {
            d: send(piece, piece, ga_s.at[3 * s + d - 1], ga_r.at[3 * s + d - 1], peer(order[0], d)[1])
            for d in ((1, 3) if s in RELAYED else (1, 3, 2))
        }
        started["out", s] = []
        pass_on(s, 0)

    def pass_on(s, d):
        piece = piece_of(s, d, 0, STREAMS[s][1] * 32)
        started["out", s].append(send(piece, piece, out_s.at[4 * s + d], out_r.at[4 * s + d], partner))

    def relay(s):
        count, order = STREAMS[s][1:]
        halves = []
        for d, low in ((1, 0), (3, count * 16)):
            started["A", s][d].wait()
            piece = piece_of(s, d, low, count * 16)
            n = 3 * s + 1 if d == 1 else 33 + s
            halves.append(send(piece, piece, ga_s.at[n], ga_r.at[n], peer(order[0], d)[1]))
            pass_on(s, d)
        started["H", s] = halves

    def finish(s):
        if s in RELAYED:
            for copy in started["H", s]:
                copy.wait()
            pass_on(s, 2)
        else:
            for d in (1, 3, 2):
                started["A", s][d].wait()
                pass_on(s, d)

    def assemble(s):
        at, count, order = STREAMS[s]
        for copy in started["out", s]:
            copy.wait()
        for tile in range(at, at + count):
            for half in range(2):
                A, B = SLOTS[half][tile]
                pick = slice(tile * N, (tile + 1) * N)
                value = full[half, pick, :] * rden[half, pick, :]
                high = value.astype(BF16)
                low = (value - high.astype(F32)) * grow[0:1, :]
                down, across = slice(A * N, (A + 1) * N), slice(B * N, (B + 1) * N)
                c_high[down, across] = high
                c_low[down, across] = low.astype(F8)
                if A < B:
                    c_high[across, down] = high.T
                    c_low[across, down] = low.astype(BF16).T.astype(F8)

    arrive(0)
    early_products()
    arrive(1)
    late_products(0)
    for copy in copies:
        copy.wait()
    table[r] = (table_y[0] + table_y[1]) + (table_y[2] + table_y[3])
    copies = [
        send(table.at[r], table.at[r], tab_s.at[5 + d], tab_r.at[5 + d], peer("z", d)[1])
        for d in range(1, 4)
    ]
    table_forward = [send(table.at[r], table.at[r], tf_s.at[0], tf_r.at[0], partner)]
    for copy in starts:
        copy.wait()
    arrive(2)
    for s in (0, 1):
        scatter_b(s)
    late_products(1)

    def table_pass(_):
        for d, copy in zip(range(1, 4), copies):
            copy.wait()
            source = ((place["z"] - d + 4) % 4) * 2 + core
            table_forward.append(send(table.at[source], table.at[source], tf_s.at[d], tf_r.at[d], partner))

    def table_done(_):
        for copy in table_forward:
            copy.wait()
        for source in range(8):
            for side in range(2):
                high, low = split(table[source, side * PART : (side + 1) * PART, :])
                at = side * HALF + source * PART
                lookup_in[at : at + PART, 0:N] = high
                lookup_in[at : at + PART, N:] = low
        most = jnp.max(jnp.max(table[...], axis=0), axis=0, keepdims=True)
        most = 2.0 * jnp.max(most, axis=1, keepdims=True)
        factor = 65536.0 * jnp.sqrt(most * most + EPS) / jnp.maximum(most, 1e-30)
        grow[...] = jnp.broadcast_to(factor, (8, N))

    def norms(item):
        half, J = item
        odd = (half + J) % 2
        right = slice(J * 2 * N, (J + 1) * 2 * N)
        picks = [tile_at(2 * i + odd) for i in range(J + 1)]
        sums_in = jnp.concatenate([lookup_in[pick, :] for pick in picks], axis=0)
        select = jnp.concatenate([lookup[pick, :] for pick in picks], axis=0)
        value = lax.rsqrt(nt(sums_in, lookup[right, :]) * nt(select, lookup_in[right, :]) + EPS)
        for i in range(J + 1):
            for k in range(2):
                tile = (2 * i + odd, 2 * J + k)
                if tile in PLACE[half]:
                    at = PLACE[half][tile]
                    rden[half, tile_at(at), :] = value[i * N : (i + 1) * N, k * N : (k + 1) * N]

    tasks = [(3.2, table_pass, 0), (4.6, table_done, 0)]
    for n, J in enumerate((2, 1, 0, 5, 4, 3)):
        tasks += [(5.3 + n, norms, (0, J)), (5.8 + n, norms, (1, J))]
    for s, start_at in zip((0, 1), (0.0, 0.1)):
        tasks += [(1.7 + start_at, spread_c, s), (6.2 + start_at, gather_b, s), (11.5 + start_at, gather_a, s)]
        if s in RELAYED:
            tasks += [(19.0 + start_at, relay, s)]
        tasks += [(21.8 + start_at, finish, s), (26.2 + start_at, assemble, s)]
    for n, s in enumerate(HELD_BACK):
        tasks.append((1.9 + n * 0.01, scatter_a, s))
    for s in range(2, len(STREAMS)):
        chunk = (s - 2) // 3
        start_at = 2.2 * chunk + 0.01 * s + (0.8 if s in HELD_BACK else 0.0)
        tasks += [(3.5 + start_at, scatter_b, s), (7.4 + start_at, spread_c, s)]
        tasks += [(11.3 + start_at, gather_b, s)]
        start_at = 2.2 * chunk + 0.01 * s
        if s in RELAYED:
            tasks += [(17.2 + start_at, gather_a, s), (21.0 + start_at, relay, s)]
            tasks += [(25.8 + start_at, finish, s), (26.0 + start_at, assemble, s)]
        else:
            tasks += [(19.6 + start_at, gather_a, s), (26 + start_at, finish, s), (28.4 + start_at, assemble, s)]
    for start_at, task, s in sorted(tasks, key=lambda item: item[0]):
        task(s)

    def times_matrix(high, low):
        wide = nn(jnp.concatenate([high, low], axis=0), c_high[...])
        return wide[0:32] + (wide[32:64] + nn(high, c_low[...]) * (1.0 / grow[0:1, 0:1]))

    def gram_of(high, low):
        return nt(high, high) + (nt(high, low) + nt(low, high))

    def solved(inverse, high, low):
        inverse_high, inverse_low = split(inverse)
        return nn(inverse_high, high) + (nn(inverse_high, low) + nn(inverse_low, high))

    wt[...] = first[...].T[0:32, :]

    def iterate(step, carry):
        high, low = split(times_matrix(*split(wt[...])))
        inverse = lower_inverse(gram_of(high, low))
        wt[...] = solved(inverse, high, low)
        return carry

    lax.fori_loop(0, ITERS, iterate, 0)
    first[:, 0:32] = (wt[...] * math.sqrt(1536)).T
    basis_out[...] = first[rows_at(here, PART), :].T[0:32, :]
    lane = jnp.minimum(here // N, 1536 // N - 2) * N
    window = pl.ds(pl.multiple_of(lane, N), 2 * N)
    shift = (2 * N - (here - lane)) % (2 * N)
    for side in range(2):
        pick = pl.ds(pl.multiple_of(side * HALF + r * PART, 32), PART)
        block = c_high[pick, window].astype(F32) + c_low[pick, window].astype(F32) * (1.0 / grow[0:1, 0:1])
        block_out[side * PART : (side + 1) * PART, :] = pltpu.roll(block, shift, 1)[:, 0:PART]


def local(coefs, tilts, start_basis):
    vmem = pl.BlockSpec(memory_space=pltpu.VMEM)
    dma = pltpu.SemaphoreType.DMA
    block, basis = pl.pallas_call(
        kernel,
        out_shape=(
            pltpu.VMEM((ROWS, PART), F32),
            pltpu.VMEM((32, PART), F32),
        ),
        in_specs=[pl.BlockSpec(memory_space=pltpu.HBM)] * 3,
        out_specs=(vmem, vmem),
        scratch_shapes=[
            pltpu.VMEM((2, 1536), jnp.int32),
            pltpu.VMEM((32, PART), F32),
            pltpu.VMEM((2, ROWS, 1024), F32),
            pltpu.VMEM((8, 2, ROWS, N), F32),
            pltpu.VMEM((8, 2, ROWS, N), F32),
            pltpu.VMEM((2, 1536, 2 * N), BF16),
            pltpu.VMEM((2, 1536, 2 * N), BF16),
            pltpu.VMEM((1536, 2 * N), F32),
            pltpu.VMEM((1536, N), F32),
            pltpu.VMEM((N, N), F32),
            pltpu.VMEM((TILES * N, N), F32),
            pltpu.VMEM((11, 3, MOST * 32, N), F32),
            pltpu.VMEM((11, 3, MOST * 8, N), F32),
            pltpu.VMEM((11, 4, MOST * 8, N), F32),
            pltpu.VMEM((11, MOST * 32, N), F32),
            pltpu.VMEM((2, TILES * N, N), F32),
            pltpu.VMEM((2, TILES * N, N), F32),
            pltpu.VMEM((4, ROWS, N), F32),
            pltpu.VMEM((4, ROWS, N), F32),
            pltpu.VMEM((8, ROWS, N), F32),
            pltpu.VMEM((1536, 2 * N), BF16),
            pltpu.VMEM((1536, 2 * N), BF16),
            pltpu.VMEM((1536, N), F32),
            pltpu.VMEM((1536, 1536), BF16),
            pltpu.VMEM((1536, 1536), F8),
            pltpu.VMEM((8, N), F32),
            pltpu.VMEM((32, 1536), F32),
            dma((3,)),
            dma((21,)), dma((21,)), dma((24,)), dma((24,)),
            dma((9,)), dma((9,)), dma((4,)), dma((4,)), dma((9,)), dma((9,)),
            dma((33,)), dma((33,)), dma((33,)), dma((33,)), dma((33,)), dma((33,)),
            dma((33,)), dma((33,)), dma((44,)), dma((44,)), dma((44,)), dma((44,)),
        ],
        compiler_params=pltpu.CompilerParams(
            collective_id=0, has_side_effects=True, vmem_limit_bytes=55296 << 10
        ),
        name="whole",
    )(coefs, tilts.T, start_basis.T)
    return block, basis.T


def solution(mesh):
    in_specs = (P(None, "row", "col"), P(), P("col", None))
    out_specs = (P("row", "col"), P("col", None))
    return jax.shard_map(local, mesh=mesh, in_specs=in_specs, out_specs=out_specs, check_vma=False)
```

```python
import math

import jax
import jax.numpy as jnp
from jax import lax
from jax.experimental import pallas as pl
from jax.experimental.pallas import tpu as pltpu
from jax.sharding import PartitionSpec as P

GRID = 32
ITERS = 4
EPS = 1e-06
MESH = pl.DeviceIdType.MESH
F32 = jnp.float32
BF16 = jnp.bfloat16
F8 = jnp.float8_e4m3fn

ROWS = 192
PART = 96
N = 128
LOW = 8
WIDE = 6

HALF = 768

SLOTS = ([], [])
for wave in ((2, 1, 0), (5, 4, 3)):
    for J in wave:
        for half in range(2):
            odd = (half + J) % 2
            SLOTS[half].extend((2 * i + odd, 2 * J + k) for i in range(J) for k in range(2))
            SLOTS[half].append((2 * J + odd, 2 * J + 1))
        if J in (0, 4, 3):
            low = J - J % 2
            SLOTS[0].append((2 * low, 2 * low))
            SLOTS[1].append((2 * low + 2, 2 * low + 2))
PLACE = [{tile: n for n, tile in enumerate(slots)} for slots in SLOTS]
TILES = len(SLOTS[0])
ORDERS = (("x", "y", "z"), ("y", "x", "z"), ("z", "x", "y"))
STREAMS = [(0, 5, ("x", "y", "z")), (5, 5, ("y", "x", "z"))]
for counts in ((4, 3, 3), (3, 4, 3), (3, 3, 3)):
    for count, order in zip(counts, ORDERS):
        STREAMS.append((STREAMS[-1][0] + STREAMS[-1][1], count, order))
MOST = 5
RELAYED = (0, 1)
HELD_BACK = (7, 10)
PANEL = 16


def nt(left, right):
    return lax.dot_general(left, right, (((1,), (1,)), ((), ())), preferred_element_type=F32)


def nn(left, right):
    return lax.dot_general(left, right, (((1,), (0,)), ((), ())), preferred_element_type=F32)


def split(value):
    high = value.astype(BF16)
    return high, (value - high.astype(F32)).astype(BF16)


def rows_at(at, size):
    return pl.ds(pl.multiple_of(at, 8), size)


def lower_inverse(gram):
    row_of = lax.broadcasted_iota(jnp.int32, (32, 32), 0)
    column_of = lax.broadcasted_iota(jnp.int32, (32, 32), 1)

    def everywhere(value):
        return jnp.broadcast_to(value, (32, 32))

    inverse = jnp.where(row_of == column_of, 1.0, 0.0).astype(F32)
    pivots = jnp.ones((32, 32), F32)
    for j in range(0, 32, PANEL):
        columns = [everywhere(gram[:, j + q : j + q + 1]) for q in range(PANEL)]
        for p in range(PANEL):
            at = slice(j + p, j + p + 1)
            pivot = everywhere(columns[p][at, :])
            pivots = jnp.where(row_of == j + p, pivot, pivots)
            factor = jnp.where(row_of > j + p, columns[p] * (1.0 / pivot), 0.0)
            for q in range(p + 1, PANEL):
                columns[q] = columns[q] - factor * everywhere(columns[q][at, :])
            gram = gram - factor * everywhere(gram[at, :])
            inverse = inverse - factor * everywhere(inverse[at, :])
    return inverse * lax.rsqrt(pivots)


def kernel(
    coefs, tilts_in, start_in,
    block_out, basis_out,
    tilts, start, held, own, other, x_high, x_low, masks, chosen, corner,
    partial, recv_a, recv_b, recv_c, acc, full, rden,
    table_x, table_y, table, lookup, lookup_in, first,
    c_high, c_low, grow, wt,
    held_s, a2a_s, a2a_r, fwd_s, fwd_r, tab_s, tab_r, tf_s, tf_r, st_s, st_r,
    ra_s, ra_r, rb_s, rb_r, rc_s, rc_r, gb_s, gb_r, ga_s, ga_r, out_s, out_r,
):
    r = lax.axis_index("row")
    c = lax.axis_index("col")
    core = r % 2
    mate = r + 1 - 2 * core
    place = {"x": c % 4, "y": c // 4, "z": r // 2}

    def peer(axis, d):
        p = (place[axis] + d) % 4
        if axis == "x":
            return p, (r, place["y"] * 4 + p)
        if axis == "y":
            return p, (r, p * 4 + place["x"])
        return p, (p * 2 + core, c)

    partner = (mate, c)

    def send(src, dst, ss, rs, device):
        copy = pltpu.make_async_remote_copy(
            src_ref=src, dst_ref=dst, send_sem=ss, recv_sem=rs,
            device_id=device, device_id_type=MESH,
        )
        copy.start()
        return copy

    barrier = pltpu.get_barrier_semaphore()
    for d in range(1, 8):
        pl.semaphore_signal(barrier, inc=1, device_id=((r + d) % 8, c), device_id_type=MESH)
    for axis in ("x", "y"):
        for d in range(1, 4):
            pl.semaphore_signal(barrier, inc=1, device_id=peer(axis, d)[1], device_id_type=MESH)
    held_copy = pltpu.make_async_copy(coefs, held, held_s.at[0])
    held_copy.start()
    small_copies = [
        pltpu.make_async_copy(start_in, start, held_s.at[1]),
        pltpu.make_async_copy(tilts_in, tilts, held_s.at[2]),
    ]
    for copy in small_copies:
        copy.start()
    mine = pl.ds(pl.multiple_of(r * N, N), N)
    corner[...] = jnp.zeros((N, N), F32)
    small_copies[0].wait()
    corner[0:32, 0:PART] = start[...]
    here = (c % 2 * 8 + c // 2) * PART
    first[rows_at(here, PART), :] = corner[...].T[0:PART, :]
    held_copy.wait()
    pl.semaphore_wait(barrier, 13)

    cuts = (
        (slice(0, 2), pl.ds(0, PART)),
        (slice(0, 1), pl.ds(PART, PART)),
        (slice(1, 2), pl.ds(PART, PART)),
    )
    exchange = ([], [], [])
    forward = ([], [], [])
    for step, (parts, rows) in enumerate(cuts):
        for n, d in enumerate((2, 6, 1, 7, 3, 5, 4)):
            p = (r + d) % 8
            n = 7 * step + n
            exchange[step].append((d, send(
                held.at[parts, rows, pl.ds(pl.multiple_of(p * N, N), N)],
                own.at[r, parts, rows], a2a_s.at[n], a2a_r.at[n], (p, c),
            )))
        forward[step].append(send(
            held.at[parts, rows, mine], other.at[r, parts, rows],
            fwd_s.at[8 * step], fwd_r.at[8 * step], partner,
        ))
    own_rows = rows_at(here, PART)
    starts = [
        send(first.at[own_rows], first.at[own_rows], st_s.at[d - 1], st_r.at[d - 1], peer("x", d)[1])
        for d in range(1, 4)
    ]

    small_copies[1].wait()
    low_side = tilts[0:1, :]
    high_side = tilts[1:2, :]
    line = lax.broadcasted_iota(jnp.int32, (N, 1536), 0)
    picked = (line == high_side - LOW) | (line == low_side - LOW + 64)
    picked = jnp.where(picked, 1.0, 0.0)
    picked = jnp.where(line == 126, low_side.astype(F32), picked)
    picked = jnp.where(line == 127, high_side.astype(F32), picked)
    picked = picked.T
    for n in range(16):
        at = (n % 2 * 8 + n // 2) * PART
        chosen[at : at + PART, :] = picked[n * PART : (n + 1) * PART, :]
    column = lax.broadcasted_iota(jnp.int32, (1536, N), 1)
    one_hot = jnp.where(column < 126, chosen[...], 0.0).astype(BF16)
    lookup[:, 0:N] = one_hot
    lookup[:, N:] = one_hot

    def waves(at, count):
        wave = at + lax.broadcasted_iota(jnp.int32, (1, count), 1)
        wave_x = jnp.abs(wave // (GRID * (GRID // 2)) - GRID // 2).astype(F32)
        wave_z = wave % GRID - GRID // 2
        return wave_x, wave_z >= 0, (jnp.abs(wave_z) * 16).astype(F32)

    def wedge(pick, wave):
        wave_x, upward, need = wave
        limit = jnp.where(upward, chosen[pick, 127:128], chosen[pick, 126:127])
        return jnp.where(need <= limit * wave_x, 1.0, 0.0)

    for side, position in enumerate((r, mate)):
        wave = waves(c * 1024 + position * N, N)
        for source in range(8):
            pick = pl.ds(source * ROWS, ROWS)
            masks[pick, side * N : (side + 1) * N] = wedge(pick, wave)

    own[r] = held[:, :, mine]

    wave = waves(c * 1024, 1024)
    wave_x, upward, need = wave
    own_mask = jnp.concatenate(
        [wedge(rows_at(r * PART, PART), wave), wedge(rows_at(HALF + r * PART, PART), wave)], axis=0
    )
    real, imag = held[0] * own_mask, held[1] * own_mask
    energy = real * real + imag * imag
    slope = lax.broadcasted_iota(jnp.int32, (N, 1), 0)
    below = need <= (slope % 64 + LOW).astype(F32) * wave_x
    side = jnp.where(slope < 64, 1, 0) == jnp.where(upward, 1, 0)
    pattern = jnp.where(below & side, 1.0, 0.0).astype(BF16)
    high = energy.astype(BF16)
    middle, low = split(energy - high.astype(F32))
    sums = nt(high, pattern) + nt(middle, pattern) + nt(low, pattern)

    def ring_send(buffer, value, axis, base):
        buffer[place[axis]] = value
        return [
            send(
                buffer.at[place[axis]], buffer.at[place[axis]],
                tab_s.at[base + d - 1], tab_r.at[base + d - 1], peer(axis, d)[1],
            )
            for d in range(1, 4)
        ]

    copies = ring_send(table_x, sums, "x", 0)
    for copy in starts:
        copy.wait()
    starts = []
    for side in range(2):
        own_rows = rows_at(side * HALF + place["y"] * 2 * PART, 2 * PART)
        for d in range(1, 4):
            n = 3 * side + d + 2
            starts.append(send(first.at[own_rows], first.at[own_rows], st_s.at[n], st_r.at[n], peer("y", d)[1]))
    for copy in copies:
        copy.wait()
    copies = ring_send(table_y, (table_x[0] + table_x[1]) + (table_x[2] + table_x[3]), "y", 3)

    def arrive(step):
        parts, rows = cuts[step]
        for n, (d, copy) in enumerate(exchange[step]):
            copy.wait()
            source = (r - d + 8) % 8
            n = 8 * step + n + 1
            forward[step].append(send(
                own.at[source, parts, rows], other.at[source, parts, rows], fwd_s.at[n], fwd_r.at[n], partner,
            ))
        base = 0 if step == 0 else HALF
        for side, ref in enumerate((own, other)):
            if side == 1:
                for copy in forward[step]:
                    copy.wait()
            lane = slice(side * N, (side + 1) * N)
            for source in range(8):
                pick = pl.ds(base + source * PART, PART)
                mask = masks[pick, lane]
                for part in range(parts.start, parts.stop):
                    high, low = split(ref[source, part, rows, :] * mask)
                    x_high[part, pick, lane] = high
                    x_low[part, pick, lane] = low

    started = {}

    def scatter(s, source, buffer, size, axis, ss, rs):
        copies = []
        for d in range(1, 4):
            p, device = peer(axis, d)
            n = 3 * s + d - 1
            copies.append(send(
                source.at[rows_at(p * size, size)],
                buffer.at[s, d - 1, pl.ds(0, size)], ss.at[n], rs.at[n], device,
            ))
        return copies

    def scatter_a(s):
        at, count, order = STREAMS[s]
        source = partial.at[pl.ds(at * N, count * N)]
        started["a", s] = scatter(s, source, recv_a, count * 32, order[0], ra_s, ra_r)

    def product(J, part):
        odd = (core + J) % 2
        right_high = x_high[part, J * 2 * N : (J + 1) * 2 * N, :]
        right_low = x_low[part, J * 2 * N : (J + 1) * 2 * N, :]
        picks = [pl.ds(pl.multiple_of((2 * i + odd) * N, N), N) for i in range(J + 1)]
        left_high = jnp.concatenate([x_high[part, pick, :] for pick in picks], axis=0)
        left_low = jnp.concatenate([x_low[part, pick, :] for pick in picks], axis=0)
        return nt(left_high, right_high) + nt(left_high, right_low) + nt(left_low, right_high)

    def cut(J, value):
        tiles = [value[i * N : (i + 1) * N, k * N : (k + 1) * N] for i in range(J + 1) for k in range(2)]
        return tiles.pop(2 * J), tiles

    def tile_at(n):
        return slice(n * N, (n + 1) * N)

    def early_products():
        at = 0
        spares = {}
        for J in (2, 1, 0):
            spares[J], tiles = cut(J, product(J, 0) + product(J, 1))
            if J == 0:
                tiles.append(jnp.where(core == 0, spares[0], spares[1]))
            for tile in tiles:
                partial[tile_at(at), :] = tile
                at += 1
        corner[...] = spares[2]
        for s in (0, 1):
            scatter_a(s)

    def late_products(part):
        at = 10
        stream = 2
        spares = {}
        for J in (5, 4, 3):
            spares[J], tiles = cut(J, product(J, part))
            if J == 4:
                tiles.append(jnp.where(core == 0, spares[4], spares[5]))
            if J == 3:
                kept = corner[...] if part == 0 else jnp.zeros((N, N), F32)
                tiles.append(jnp.where(core == 0, kept, spares[3]))
            for tile in tiles:
                if part == 0:
                    partial[tile_at(at), :] = tile
                else:
                    partial[tile_at(at), :] += tile
                at += 1
            while part == 1 and stream < len(STREAMS) and sum(STREAMS[stream][:2]) <= at:
                if stream not in HELD_BACK:
                    scatter_a(stream)
                stream += 1

    def scatter_b(s):
        count, order = STREAMS[s][1:]
        size = count * 32
        for copy in started["a", s]:
            copy.wait()
        pick = rows_at(STREAMS[s][0] * N + place[order[0]] * size, size)
        got = [recv_a[s, n, 0:size, :] for n in range(3)]
        acc[s, 0:size, :] = (partial[pick, :] + got[0]) + (got[1] + got[2])
        started["b", s] = scatter(s, acc.at[s], recv_b, count * 8, order[1], rb_s, rb_r)

    def spread_c(s):
        count, order = STREAMS[s][1:]
        size = count * 8
        for copy in started["b", s]:
            copy.wait()
        got = [recv_b[s, n, 0:size, :] for n in range(3)]
        value = (acc[s, rows_at(place[order[1]] * size, size), :] + got[0]) + (got[1] + got[2])
        here = place[order[2]]
        recv_c[s, here, 0:size, :] = value
        piece = recv_c.at[s, here, pl.ds(0, size)]
        started["c", s] = [
            send(piece, piece, rc_s.at[3 * s + d - 1], rc_r.at[3 * s + d - 1], peer(order[2], d)[1])
            for d in range(1, 4)
        ]

    def gather_b(s):
        at, count, order = STREAMS[s]
        size = count * 8
        for copy in started["c", s]:
            copy.wait()
        got = [recv_c[s, n, 0:size, :] for n in range(4)]
        pick = rows_at(at * N + (place[order[0]] * 4 + place[order[1]]) * size, size)
        full[core, pick, :] = (got[0] + got[1]) + (got[2] + got[3])
        piece = full.at[core, pick]
        started["B", s] = [
            send(piece, piece, gb_s.at[3 * s + d - 1], gb_r.at[3 * s + d - 1], peer(order[1], d)[1])
            for d in range(1, 4)
        ]

    def piece_of(s, d, low, size):
        at, count, order = STREAMS[s]
        seg = (place[order[0]] - d + 4) % 4 * count * 32
        return full.at[core, rows_at(at * N + seg + low, size)]

    def gather_a(s):
        count, order = STREAMS[s][1:]
        for copy in started["B", s]:
            copy.wait()
        piece = piece_of(s, 0, 0, count * 32)
        started["A", s] = {
            d: send(piece, piece, ga_s.at[3 * s + d - 1], ga_r.at[3 * s + d - 1], peer(order[0], d)[1])
            for d in ((1, 3) if s in RELAYED else (1, 3, 2))
        }
        started["out", s] = []
        pass_on(s, 0)

    def pass_on(s, d):
        piece = piece_of(s, d, 0, STREAMS[s][1] * 32)
        started["out", s].append(send(piece, piece, out_s.at[4 * s + d], out_r.at[4 * s + d], partner))

    def relay(s):
        count, order = STREAMS[s][1:]
        halves = []
        for d, low in ((1, 0), (3, count * 16)):
            started["A", s][d].wait()
            piece = piece_of(s, d, low, count * 16)
            n = 3 * s + 1 if d == 1 else 33 + s
            halves.append(send(piece, piece, ga_s.at[n], ga_r.at[n], peer(order[0], d)[1]))
            pass_on(s, d)
        started["H", s] = halves

    def finish(s):
        if s in RELAYED:
            for copy in started["H", s]:
                copy.wait()
            pass_on(s, 2)
        else:
            for d in (1, 3, 2):
                started["A", s][d].wait()
                pass_on(s, d)

    def assemble(s):
        at, count, order = STREAMS[s]
        for copy in started["out", s]:
            copy.wait()
        for tile in range(at, at + count):
            for half in range(2):
                A, B = SLOTS[half][tile]
                pick = slice(tile * N, (tile + 1) * N)
                value = full[half, pick, :] * rden[half, pick, :]
                high = value.astype(BF16)
                low = (value - high.astype(F32)) * grow[0:1, :]
                down, across = slice(A * N, (A + 1) * N), slice(B * N, (B + 1) * N)
                c_high[down, across] = high
                c_low[down, across] = low.astype(F8)
                if A < B:
                    c_high[across, down] = high.T
                    c_low[across, down] = low.astype(BF16).T.astype(F8)

    arrive(0)
    early_products()
    arrive(1)
    late_products(0)
    for copy in copies:
        copy.wait()
    table[r] = (table_y[0] + table_y[1]) + (table_y[2] + table_y[3])
    copies = [
        send(table.at[r], table.at[r], tab_s.at[5 + d], tab_r.at[5 + d], peer("z", d)[1])
        for d in range(1, 4)
    ]
    table_forward = [send(table.at[r], table.at[r], tf_s.at[0], tf_r.at[0], partner)]
    for copy in starts:
        copy.wait()
    arrive(2)
    for s in (0, 1):
        scatter_b(s)
    late_products(1)

    def table_pass(_):
        for d, copy in zip(range(1, 4), copies):
            copy.wait()
            source = ((place["z"] - d + 4) % 4) * 2 + core
            table_forward.append(send(table.at[source], table.at[source], tf_s.at[d], tf_r.at[d], partner))

    def table_done(_):
        for copy in table_forward:
            copy.wait()
        for source in range(8):
            for side in range(2):
                high, low = split(table[source, side * PART : (side + 1) * PART, :])
                at = side * HALF + source * PART
                lookup_in[at : at + PART, 0:N] = high
                lookup_in[at : at + PART, N:] = low
        most = jnp.max(jnp.max(table[...], axis=0), axis=0, keepdims=True)
        most = 2.0 * jnp.max(most, axis=1, keepdims=True)
        factor = 65536.0 * jnp.sqrt(most * most + EPS) / jnp.maximum(most, 1e-30)
        grow[...] = jnp.broadcast_to(factor, (8, N))

    def norms(item):
        half, J = item
        odd = (half + J) % 2
        right = slice(J * 2 * N, (J + 1) * 2 * N)
        picks = [tile_at(2 * i + odd) for i in range(J + 1)]
        sums_in = jnp.concatenate([lookup_in[pick, :] for pick in picks], axis=0)
        select = jnp.concatenate([lookup[pick, :] for pick in picks], axis=0)
        value = lax.rsqrt(nt(sums_in, lookup[right, :]) * nt(select, lookup_in[right, :]) + EPS)
        for i in range(J + 1):
            for k in range(2):
                tile = (2 * i + odd, 2 * J + k)
                if tile in PLACE[half]:
                    at = PLACE[half][tile]
                    rden[half, tile_at(at), :] = value[i * N : (i + 1) * N, k * N : (k + 1) * N]

    tasks = [(3.2, table_pass, 0), (4.6, table_done, 0)]
    for n, J in enumerate((2, 1, 0, 5, 4, 3)):
        tasks += [(5.3 + n, norms, (0, J)), (5.8 + n, norms, (1, J))]
    for s, start_at in zip((0, 1), (0.0, 0.1)):
        tasks += [(1.7 + start_at, spread_c, s), (6.2 + start_at, gather_b, s), (10.5 + start_at, gather_a, s)]
        if s in RELAYED:
            tasks += [(19.0 + start_at, relay, s)]
        tasks += [(21.8 + start_at, finish, s), (26.2 + start_at, assemble, s)]
    for n, s in enumerate(HELD_BACK):
        tasks.append((1.9 + n * 0.01, scatter_a, s))
    for s in range(2, len(STREAMS)):
        chunk = (s - 2) // 3
        start_at = 2.2 * chunk + 0.01 * s + (0.8 if s in HELD_BACK else 0.0)
        tasks += [(3.5 + start_at, scatter_b, s), (7.4 + start_at, spread_c, s)]
        tasks += [(11.3 + start_at, gather_b, s)]
        start_at = 2.2 * chunk + 0.01 * s
        if s in RELAYED:
            tasks += [(17.2 + start_at, gather_a, s), (21.0 + start_at, relay, s)]
            tasks += [(25.8 + start_at, finish, s), (26.0 + start_at, assemble, s)]
        else:
            tasks += [(19.6 + start_at, gather_a, s), (26 + start_at, finish, s), (28.4 + start_at, assemble, s)]
    for start_at, task, s in sorted(tasks, key=lambda item: item[0]):
        task(s)

    def times_matrix(high, low):
        wide = nn(jnp.concatenate([high, low], axis=0), c_high[...])
        return wide[0:32] + (wide[32:64] + nn(high, c_low[...]) * (1.0 / grow[0:1, 0:1]))

    def gram_of(high, low):
        return nt(high, high) + (nt(high, low) + nt(low, high))

    def solved(inverse, high, low):
        inverse_high, inverse_low = split(inverse)
        return nn(inverse_high, high) + (nn(inverse_high, low) + nn(inverse_low, high))

    wt[...] = first[...].T[0:32, :]

    def iterate(step, carry):
        high, low = split(times_matrix(*split(wt[...])))
        inverse = lower_inverse(gram_of(high, low))
        wt[...] = solved(inverse, high, low)
        return carry

    lax.fori_loop(0, ITERS, iterate, 0)
    first[:, 0:32] = (wt[...] * math.sqrt(1536)).T
    basis_out[...] = first[rows_at(here, PART), :].T[0:32, :]
    lane = jnp.minimum(here // N, 1536 // N - 2) * N
    window = pl.ds(pl.multiple_of(lane, N), 2 * N)
    shift = (2 * N - (here - lane)) % (2 * N)
    for side in range(2):
        pick = pl.ds(pl.multiple_of(side * HALF + r * PART, 32), PART)
        block = c_high[pick, window].astype(F32) + c_low[pick, window].astype(F32) * (1.0 / grow[0:1, 0:1])
        block_out[side * PART : (side + 1) * PART, :] = pltpu.roll(block, shift, 1)[:, 0:PART]


def local(coefs, tilts, start_basis):
    vmem = pl.BlockSpec(memory_space=pltpu.VMEM)
    dma = pltpu.SemaphoreType.DMA
    block, basis = pl.pallas_call(
        kernel,
        out_shape=(
            pltpu.VMEM((ROWS, PART), F32),
            pltpu.VMEM((32, PART), F32),
        ),
        in_specs=[pl.BlockSpec(memory_space=pltpu.HBM)] * 3,
        out_specs=(vmem, vmem),
        scratch_shapes=[
            pltpu.VMEM((2, 1536), jnp.int32),
            pltpu.VMEM((32, PART), F32),
            pltpu.VMEM((2, ROWS, 1024), F32),
            pltpu.VMEM((8, 2, ROWS, N), F32),
            pltpu.VMEM((8, 2, ROWS, N), F32),
            pltpu.VMEM((2, 1536, 2 * N), BF16),
            pltpu.VMEM((2, 1536, 2 * N), BF16),
            pltpu.VMEM((1536, 2 * N), F32),
            pltpu.VMEM((1536, N), F32),
            pltpu.VMEM((N, N), F32),
            pltpu.VMEM((TILES * N, N), F32),
            pltpu.VMEM((11, 3, MOST * 32, N), F32),
            pltpu.VMEM((11, 3, MOST * 8, N), F32),
            pltpu.VMEM((11, 4, MOST * 8, N), F32),
            pltpu.VMEM((11, MOST * 32, N), F32),
            pltpu.VMEM((2, TILES * N, N), F32),
            pltpu.VMEM((2, TILES * N, N), F32),
            pltpu.VMEM((4, ROWS, N), F32),
            pltpu.VMEM((4, ROWS, N), F32),
            pltpu.VMEM((8, ROWS, N), F32),
            pltpu.VMEM((1536, 2 * N), BF16),
            pltpu.VMEM((1536, 2 * N), BF16),
            pltpu.VMEM((1536, N), F32),
            pltpu.VMEM((1536, 1536), BF16),
            pltpu.VMEM((1536, 1536), F8),
            pltpu.VMEM((8, N), F32),
            pltpu.VMEM((32, 1536), F32),
            dma((3,)),
            dma((21,)), dma((21,)), dma((24,)), dma((24,)),
            dma((9,)), dma((9,)), dma((4,)), dma((4,)), dma((9,)), dma((9,)),
            dma((33,)), dma((33,)), dma((33,)), dma((33,)), dma((33,)), dma((33,)),
            dma((33,)), dma((33,)), dma((44,)), dma((44,)), dma((44,)), dma((44,)),
        ],
        compiler_params=pltpu.CompilerParams(
            collective_id=0, has_side_effects=True, vmem_limit_bytes=55296 << 10
        ),
        name="whole",
    )(coefs, tilts.T, start_basis.T)
    return block, basis.T


def solution(mesh):
    in_specs = (P(None, "row", "col"), P(), P("col", None))
    out_specs = (P("row", "col"), P("col", None))
    return jax.shard_map(local, mesh=mesh, in_specs=in_specs, out_specs=out_specs, check_vma=False)
```

```python
import math

import jax
import jax.numpy as jnp
from jax import lax
from jax.experimental import pallas as pl
from jax.experimental.pallas import tpu as pltpu
from jax.sharding import PartitionSpec as P

GRID = 32
ITERS = 4
EPS = 1e-06
MESH = pl.DeviceIdType.MESH
F32 = jnp.float32
BF16 = jnp.bfloat16
F8 = jnp.float8_e4m3fn

ROWS = 192
PART = 96
N = 128
LOW = 8
WIDE = 6

HALF = 768

SLOTS = ([], [])
for wave in ((2, 1, 0), (5, 4, 3)):
    for J in wave:
        for half in range(2):
            odd = (half + J) % 2
            SLOTS[half].extend((2 * i + odd, 2 * J + k) for i in range(J) for k in range(2))
            SLOTS[half].append((2 * J + odd, 2 * J + 1))
        if J in (0, 4, 3):
            low = J - J % 2
            SLOTS[0].append((2 * low, 2 * low))
            SLOTS[1].append((2 * low + 2, 2 * low + 2))
PLACE = [{tile: n for n, tile in enumerate(slots)} for slots in SLOTS]
TILES = len(SLOTS[0])
ORDERS = (("x", "y", "z"), ("y", "x", "z"), ("z", "x", "y"))
STREAMS = [(0, 5, ("x", "y", "z")), (5, 5, ("y", "x", "z"))]
for counts in ((4, 3, 3), (3, 4, 3), (3, 3, 3)):
    for count, order in zip(counts, ORDERS):
        STREAMS.append((STREAMS[-1][0] + STREAMS[-1][1], count, order))
MOST = 5
RELAYED = (0, 1)
HELD_BACK = (7, 10)
PANEL = 16


def nt(left, right):
    return lax.dot_general(left, right, (((1,), (1,)), ((), ())), preferred_element_type=F32)


def nn(left, right):
    return lax.dot_general(left, right, (((1,), (0,)), ((), ())), preferred_element_type=F32)


def split(value):
    high = value.astype(BF16)
    return high, (value - high.astype(F32)).astype(BF16)


def rows_at(at, size):
    return pl.ds(pl.multiple_of(at, 8), size)


def lower_inverse(gram):
    row_of = lax.broadcasted_iota(jnp.int32, (32, 32), 0)
    column_of = lax.broadcasted_iota(jnp.int32, (32, 32), 1)

    def everywhere(value):
        return jnp.broadcast_to(value, (32, 32))

    inverse = jnp.where(row_of == column_of, 1.0, 0.0).astype(F32)
    pivots = jnp.ones((32, 32), F32)
    for j in range(0, 32, PANEL):
        columns = [everywhere(gram[:, j + q : j + q + 1]) for q in range(PANEL)]
        for p in range(PANEL):
            at = slice(j + p, j + p + 1)
            pivot = everywhere(columns[p][at, :])
            pivots = jnp.where(row_of == j + p, pivot, pivots)
            factor = jnp.where(row_of > j + p, columns[p] * (1.0 / pivot), 0.0)
            for q in range(p + 1, PANEL):
                columns[q] = columns[q] - factor * everywhere(columns[q][at, :])
            gram = gram - factor * everywhere(gram[at, :])
            inverse = inverse - factor * everywhere(inverse[at, :])
    return inverse * lax.rsqrt(pivots)


def kernel(
    coefs, tilts_in, start_in,
    block_out, basis_out,
    tilts, start, held, own, other, x_high, x_low, masks, chosen, corner,
    partial, recv_a, recv_b, recv_c, acc, full, rden,
    table_x, table_y, table, lookup, lookup_in, first,
    c_high, c_low, grow, wt,
    held_s, a2a_s, a2a_r, fwd_s, fwd_r, tab_s, tab_r, tf_s, tf_r, st_s, st_r,
    ra_s, ra_r, rb_s, rb_r, rc_s, rc_r, gb_s, gb_r, ga_s, ga_r, out_s, out_r,
):
    r = lax.axis_index("row")
    c = lax.axis_index("col")
    core = r % 2
    mate = r + 1 - 2 * core
    place = {"x": c % 4, "y": c // 4, "z": r // 2}

    def peer(axis, d):
        p = (place[axis] + d) % 4
        if axis == "x":
            return p, (r, place["y"] * 4 + p)
        if axis == "y":
            return p, (r, p * 4 + place["x"])
        return p, (p * 2 + core, c)

    partner = (mate, c)

    def send(src, dst, ss, rs, device):
        copy = pltpu.make_async_remote_copy(
            src_ref=src, dst_ref=dst, send_sem=ss, recv_sem=rs,
            device_id=device, device_id_type=MESH,
        )
        copy.start()
        return copy

    barrier = pltpu.get_barrier_semaphore()
    for d in range(1, 8):
        pl.semaphore_signal(barrier, inc=1, device_id=((r + d) % 8, c), device_id_type=MESH)
    for axis in ("x", "y"):
        for d in range(1, 4):
            pl.semaphore_signal(barrier, inc=1, device_id=peer(axis, d)[1], device_id_type=MESH)
    held_copy = pltpu.make_async_copy(coefs, held, held_s.at[0])
    held_copy.start()
    small_copies = [
        pltpu.make_async_copy(start_in, start, held_s.at[1]),
        pltpu.make_async_copy(tilts_in, tilts, held_s.at[2]),
    ]
    for copy in small_copies:
        copy.start()
    mine = pl.ds(pl.multiple_of(r * N, N), N)
    corner[...] = jnp.zeros((N, N), F32)
    small_copies[0].wait()
    corner[0:32, 0:PART] = start[...]
    here = (c % 2 * 8 + c // 2) * PART
    first[rows_at(here, PART), :] = corner[...].T[0:PART, :]
    held_copy.wait()
    pl.semaphore_wait(barrier, 13)

    cuts = (
        (slice(0, 2), pl.ds(0, PART)),
        (slice(0, 1), pl.ds(PART, PART)),
        (slice(1, 2), pl.ds(PART, PART)),
    )
    exchange = ([], [], [])
    forward = ([], [], [])
    for step, (parts, rows) in enumerate(cuts):
        for n, d in enumerate((2, 6, 1, 7, 3, 5, 4)):
            p = (r + d) % 8
            n = 7 * step + n
            exchange[step].append((d, send(
                held.at[parts, rows, pl.ds(pl.multiple_of(p * N, N), N)],
                own.at[r, parts, rows], a2a_s.at[n], a2a_r.at[n], (p, c),
            )))
        forward[step].append(send(
            held.at[parts, rows, mine], other.at[r, parts, rows],
            fwd_s.at[8 * step], fwd_r.at[8 * step], partner,
        ))
    own_rows = rows_at(here, PART)
    starts = [
        send(first.at[own_rows], first.at[own_rows], st_s.at[d - 1], st_r.at[d - 1], peer("x", d)[1])
        for d in range(1, 4)
    ]

    small_copies[1].wait()
    low_side = tilts[0:1, :]
    high_side = tilts[1:2, :]
    line = lax.broadcasted_iota(jnp.int32, (N, 1536), 0)
    picked = (line == high_side - LOW) | (line == low_side - LOW + 64)
    picked = jnp.where(picked, 1.0, 0.0)
    picked = jnp.where(line == 126, low_side.astype(F32), picked)
    picked = jnp.where(line == 127, high_side.astype(F32), picked)
    picked = picked.T
    for n in range(16):
        at = (n % 2 * 8 + n // 2) * PART
        chosen[at : at + PART, :] = picked[n * PART : (n + 1) * PART, :]
    column = lax.broadcasted_iota(jnp.int32, (1536, N), 1)
    one_hot = jnp.where(column < 126, chosen[...], 0.0).astype(BF16)
    lookup[:, 0:N] = one_hot
    lookup[:, N:] = one_hot

    def waves(at, count):
        wave = at + lax.broadcasted_iota(jnp.int32, (1, count), 1)
        wave_x = jnp.abs(wave // (GRID * (GRID // 2)) - GRID // 2).astype(F32)
        wave_z = wave % GRID - GRID // 2
        return wave_x, wave_z >= 0, (jnp.abs(wave_z) * 16).astype(F32)

    def wedge(pick, wave):
        wave_x, upward, need = wave
        limit = jnp.where(upward, chosen[pick, 127:128], chosen[pick, 126:127])
        return jnp.where(need <= limit * wave_x, 1.0, 0.0)

    for side, position in enumerate((r, mate)):
        wave = waves(c * 1024 + position * N, N)
        for source in range(8):
            pick = pl.ds(source * ROWS, ROWS)
            masks[pick, side * N : (side + 1) * N] = wedge(pick, wave)

    own[r] = held[:, :, mine]

    wave = waves(c * 1024, 1024)
    wave_x, upward, need = wave
    own_mask = jnp.concatenate(
        [wedge(rows_at(r * PART, PART), wave), wedge(rows_at(HALF + r * PART, PART), wave)], axis=0
    )
    real, imag = held[0] * own_mask, held[1] * own_mask
    energy = real * real + imag * imag
    slope = lax.broadcasted_iota(jnp.int32, (N, 1), 0)
    below = need <= (slope % 64 + LOW).astype(F32) * wave_x
    side = jnp.where(slope < 64, 1, 0) == jnp.where(upward, 1, 0)
    pattern = jnp.where(below & side, 1.0, 0.0).astype(BF16)
    high = energy.astype(BF16)
    middle, low = split(energy - high.astype(F32))
    sums = nt(high, pattern) + nt(middle, pattern) + nt(low, pattern)

    def ring_send(buffer, value, axis, base):
        buffer[place[axis]] = value
        return [
            send(
                buffer.at[place[axis]], buffer.at[place[axis]],
                tab_s.at[base + d - 1], tab_r.at[base + d - 1], peer(axis, d)[1],
            )
            for d in range(1, 4)
        ]

    copies = ring_send(table_x, sums, "x", 0)
    for copy in starts:
        copy.wait()
    starts = []
    for side in range(2):
        own_rows = rows_at(side * HALF + place["y"] * 2 * PART, 2 * PART)
        for d in range(1, 4):
            n = 3 * side + d + 2
            starts.append(send(first.at[own_rows], first.at[own_rows], st_s.at[n], st_r.at[n], peer("y", d)[1]))
    for copy in copies:
        copy.wait()
    copies = ring_send(table_y, (table_x[0] + table_x[1]) + (table_x[2] + table_x[3]), "y", 3)

    def arrive(step):
        parts, rows = cuts[step]
        for n, (d, copy) in enumerate(exchange[step]):
            copy.wait()
            source = (r - d + 8) % 8
            n = 8 * step + n + 1
            forward[step].append(send(
                own.at[source, parts, rows], other.at[source, parts, rows], fwd_s.at[n], fwd_r.at[n], partner,
            ))
        base = 0 if step == 0 else HALF
        for side, ref in enumerate((own, other)):
            if side == 1:
                for copy in forward[step]:
                    copy.wait()
            lane = slice(side * N, (side + 1) * N)
            for source in range(8):
                pick = pl.ds(base + source * PART, PART)
                mask = masks[pick, lane]
                for part in range(parts.start, parts.stop):
                    high, low = split(ref[source, part, rows, :] * mask)
                    x_high[part, pick, lane] = high
                    x_low[part, pick, lane] = low

    started = {}

    def scatter(s, source, buffer, size, axis, ss, rs):
        copies = []
        for d in range(1, 4):
            p, device = peer(axis, d)
            n = 3 * s + d - 1
            copies.append(send(
                source.at[rows_at(p * size, size)],
                buffer.at[s, d - 1, pl.ds(0, size)], ss.at[n], rs.at[n], device,
            ))
        return copies

    def scatter_a(s):
        at, count, order = STREAMS[s]
        source = partial.at[pl.ds(at * N, count * N)]
        started["a", s] = scatter(s, source, recv_a, count * 32, order[0], ra_s, ra_r)

    def product(J, part):
        odd = (core + J) % 2
        right_high = x_high[part, J * 2 * N : (J + 1) * 2 * N, :]
        right_low = x_low[part, J * 2 * N : (J + 1) * 2 * N, :]
        picks = [pl.ds(pl.multiple_of((2 * i + odd) * N, N), N) for i in range(J + 1)]
        left_high = jnp.concatenate([x_high[part, pick, :] for pick in picks], axis=0)
        left_low = jnp.concatenate([x_low[part, pick, :] for pick in picks], axis=0)
        return nt(left_high, right_high) + nt(left_high, right_low) + nt(left_low, right_high)

    def cut(J, value):
        tiles = [value[i * N : (i + 1) * N, k * N : (k + 1) * N] for i in range(J + 1) for k in range(2)]
        return tiles.pop(2 * J), tiles

    def tile_at(n):
        return slice(n * N, (n + 1) * N)

    def early_products():
        at = 0
        spares = {}
        for J in (2, 1, 0):
            spares[J], tiles = cut(J, product(J, 0) + product(J, 1))
            if J == 0:
                tiles.append(jnp.where(core == 0, spares[0], spares[1]))
            for tile in tiles:
                partial[tile_at(at), :] = tile
                at += 1
        corner[...] = spares[2]
        for s in (0, 1):
            scatter_a(s)

    def late_products(part):
        at = 10
        stream = 2
        spares = {}
        for J in (5, 4, 3):
            spares[J], tiles = cut(J, product(J, part))
            if J == 4:
                tiles.append(jnp.where(core == 0, spares[4], spares[5]))
            if J == 3:
                kept = corner[...] if part == 0 else jnp.zeros((N, N), F32)
                tiles.append(jnp.where(core == 0, kept, spares[3]))
            for tile in tiles:
                if part == 0:
                    partial[tile_at(at), :] = tile
                else:
                    partial[tile_at(at), :] += tile
                at += 1
            while part == 1 and stream < len(STREAMS) and sum(STREAMS[stream][:2]) <= at:
                if stream not in HELD_BACK:
                    scatter_a(stream)
                stream += 1

    def scatter_b(s):
        count, order = STREAMS[s][1:]
        size = count * 32
        for copy in started["a", s]:
            copy.wait()
        pick = rows_at(STREAMS[s][0] * N + place[order[0]] * size, size)
        got = [recv_a[s, n, 0:size, :] for n in range(3)]
        acc[s, 0:size, :] = (partial[pick, :] + got[0]) + (got[1] + got[2])
        started["b", s] = scatter(s, acc.at[s], recv_b, count * 8, order[1], rb_s, rb_r)

    def spread_c(s):
        count, order = STREAMS[s][1:]
        size = count * 8
        for copy in started["b", s]:
            copy.wait()
        got = [recv_b[s, n, 0:size, :] for n in range(3)]
        value = (acc[s, rows_at(place[order[1]] * size, size), :] + got[0]) + (got[1] + got[2])
        here = place[order[2]]
        recv_c[s, here, 0:size, :] = value
        piece = recv_c.at[s, here, pl.ds(0, size)]
        started["c", s] = [
            send(piece, piece, rc_s.at[3 * s + d - 1], rc_r.at[3 * s + d - 1], peer(order[2], d)[1])
            for d in range(1, 4)
        ]

    def gather_b(s):
        at, count, order = STREAMS[s]
        size = count * 8
        for copy in started["c", s]:
            copy.wait()
        got = [recv_c[s, n, 0:size, :] for n in range(4)]
        pick = rows_at(at * N + (place[order[0]] * 4 + place[order[1]]) * size, size)
        full[core, pick, :] = (got[0] + got[1]) + (got[2] + got[3])
        piece = full.at[core, pick]
        started["B", s] = [
            send(piece, piece, gb_s.at[3 * s + d - 1], gb_r.at[3 * s + d - 1], peer(order[1], d)[1])
            for d in range(1, 4)
        ]

    def piece_of(s, d, low, size):
        at, count, order = STREAMS[s]
        seg = (place[order[0]] - d + 4) % 4 * count * 32
        return full.at[core, rows_at(at * N + seg + low, size)]

    def gather_a(s):
        count, order = STREAMS[s][1:]
        for copy in started["B", s]:
            copy.wait()
        piece = piece_of(s, 0, 0, count * 32)
        started["A", s] = {
            d: send(piece, piece, ga_s.at[3 * s + d - 1], ga_r.at[3 * s + d - 1], peer(order[0], d)[1])
            for d in ((1, 3) if s in RELAYED else (1, 3, 2))
        }
        started["out", s] = []
        pass_on(s, 0)

    def pass_on(s, d):
        piece = piece_of(s, d, 0, STREAMS[s][1] * 32)
        started["out", s].append(send(piece, piece, out_s.at[4 * s + d], out_r.at[4 * s + d], partner))

    def relay(s):
        count, order = STREAMS[s][1:]
        halves = []
        for d, low in ((1, 0), (3, count * 16)):
            started["A", s][d].wait()
            piece = piece_of(s, d, low, count * 16)
            n = 3 * s + 1 if d == 1 else 33 + s
            halves.append(send(piece, piece, ga_s.at[n], ga_r.at[n], peer(order[0], d)[1]))
            pass_on(s, d)
        started["H", s] = halves

    def finish(s):
        if s in RELAYED:
            for copy in started["H", s]:
                copy.wait()
            pass_on(s, 2)
        else:
            for d in (1, 3, 2):
                started["A", s][d].wait()
                pass_on(s, d)

    def assemble(s):
        at, count, order = STREAMS[s]
        for copy in started["out", s]:
            copy.wait()
        for tile in range(at, at + count):
            for half in range(2):
                A, B = SLOTS[half][tile]
                pick = slice(tile * N, (tile + 1) * N)
                value = full[half, pick, :] * rden[half, pick, :]
                high = value.astype(BF16)
                low = (value - high.astype(F32)) * grow[0:1, :]
                down, across = slice(A * N, (A + 1) * N), slice(B * N, (B + 1) * N)
                c_high[down, across] = high
                c_low[down, across] = low.astype(F8)
                if A < B:
                    c_high[across, down] = high.T
                    c_low[across, down] = low.astype(BF16).T.astype(F8)

    arrive(0)
    early_products()
    arrive(1)
    late_products(0)
    for copy in copies:
        copy.wait()
    table[r] = (table_y[0] + table_y[1]) + (table_y[2] + table_y[3])
    copies = [
        send(table.at[r], table.at[r], tab_s.at[5 + d], tab_r.at[5 + d], peer("z", d)[1])
        for d in range(1, 4)
    ]
    table_forward = [send(table.at[r], table.at[r], tf_s.at[0], tf_r.at[0], partner)]
    for copy in starts:
        copy.wait()
    arrive(2)
    for s in (0, 1):
        scatter_b(s)
    late_products(1)

    def table_pass(_):
        for d, copy in zip(range(1, 4), copies):
            copy.wait()
            source = ((place["z"] - d + 4) % 4) * 2 + core
            table_forward.append(send(table.at[source], table.at[source], tf_s.at[d], tf_r.at[d], partner))

    def table_done(_):
        for copy in table_forward:
            copy.wait()
        for source in range(8):
            for side in range(2):
                high, low = split(table[source, side * PART : (side + 1) * PART, :])
                at = side * HALF + source * PART
                lookup_in[at : at + PART, 0:N] = high
                lookup_in[at : at + PART, N:] = low
        most = jnp.max(jnp.max(table[...], axis=0), axis=0, keepdims=True)
        most = 2.0 * jnp.max(most, axis=1, keepdims=True)
        factor = 65536.0 * jnp.sqrt(most * most + EPS) / jnp.maximum(most, 1e-30)
        grow[...] = jnp.broadcast_to(factor, (8, N))

    def norms(item):
        half, J = item
        odd = (half + J) % 2
        right = slice(J * 2 * N, (J + 1) * 2 * N)
        picks = [tile_at(2 * i + odd) for i in range(J + 1)]
        sums_in = jnp.concatenate([lookup_in[pick, :] for pick in picks], axis=0)
        select = jnp.concatenate([lookup[pick, :] for pick in picks], axis=0)
        value = lax.rsqrt(nt(sums_in, lookup[right, :]) * nt(select, lookup_in[right, :]) + EPS)
        for i in range(J + 1):
            for k in range(2):
                tile = (2 * i + odd, 2 * J + k)
                if tile in PLACE[half]:
                    at = PLACE[half][tile]
                    rden[half, tile_at(at), :] = value[i * N : (i + 1) * N, k * N : (k + 1) * N]

    tasks = [(3.2, table_pass, 0), (4.6, table_done, 0)]
    for n, J in enumerate((2, 1, 0, 5, 4, 3)):
        tasks += [(5.3 + n, norms, (0, J)), (5.8 + n, norms, (1, J))]
    for s, start_at in zip((0, 1), (0.0, 0.1)):
        tasks += [(1.7 + start_at, spread_c, s), (6.2 + start_at, gather_b, s), (10.5 + start_at, gather_a, s)]
        if s in RELAYED:
            tasks += [(19.0 + start_at, relay, s)]
        tasks += [(21.8 + start_at, finish, s), (26.2 + start_at, assemble, s)]
    for n, s in enumerate(HELD_BACK):
        tasks.append((1.9 + n * 0.01, scatter_a, s))
    for s in range(2, len(STREAMS)):
        chunk = (s - 2) // 3
        start_at = 2.2 * chunk + 0.01 * s + (0.8 if s in HELD_BACK else 0.0)
        tasks += [(3.5 + start_at, scatter_b, s), (7.4 + start_at, spread_c, s)]
        tasks += [(11.3 + start_at, gather_b, s)]
        start_at = 2.2 * chunk + 0.01 * s
        if s in RELAYED:
            tasks += [(17.2 + start_at, gather_a, s), (21.0 + start_at, relay, s)]
            tasks += [(25.8 + start_at, finish, s), (26.0 + start_at, assemble, s)]
        else:
            tasks += [((15.7, 21.8, 24.0)[chunk] + 0.01 * s, gather_a, s), (26 + start_at, finish, s), (28.4 + start_at, assemble, s)]
    for start_at, task, s in sorted(tasks, key=lambda item: item[0]):
        task(s)

    def times_matrix(high, low):
        wide = nn(jnp.concatenate([high, low], axis=0), c_high[...])
        return wide[0:32] + (wide[32:64] + nn(high, c_low[...]) * (1.0 / grow[0:1, 0:1]))

    def gram_of(high, low):
        return nt(high, high) + (nt(high, low) + nt(low, high))

    def solved(inverse, high, low):
        inverse_high, inverse_low = split(inverse)
        return nn(inverse_high, high) + (nn(inverse_high, low) + nn(inverse_low, high))

    wt[...] = first[...].T[0:32, :]

    def iterate(step, carry):
        high, low = split(times_matrix(*split(wt[...])))
        inverse = lower_inverse(gram_of(high, low))
        wt[...] = solved(inverse, high, low)
        return carry

    lax.fori_loop(0, ITERS, iterate, 0)
    first[:, 0:32] = (wt[...] * math.sqrt(1536)).T
    basis_out[...] = first[rows_at(here, PART), :].T[0:32, :]
    lane = jnp.minimum(here // N, 1536 // N - 2) * N
    window = pl.ds(pl.multiple_of(lane, N), 2 * N)
    shift = (2 * N - (here - lane)) % (2 * N)
    for side in range(2):
        pick = pl.ds(pl.multiple_of(side * HALF + r * PART, 32), PART)
        block = c_high[pick, window].astype(F32) + c_low[pick, window].astype(F32) * (1.0 / grow[0:1, 0:1])
        block_out[side * PART : (side + 1) * PART, :] = pltpu.roll(block, shift, 1)[:, 0:PART]


def local(coefs, tilts, start_basis):
    vmem = pl.BlockSpec(memory_space=pltpu.VMEM)
    dma = pltpu.SemaphoreType.DMA
    block, basis = pl.pallas_call(
        kernel,
        out_shape=(
            pltpu.VMEM((ROWS, PART), F32),
            pltpu.VMEM((32, PART), F32),
        ),
        in_specs=[pl.BlockSpec(memory_space=pltpu.HBM)] * 3,
        out_specs=(vmem, vmem),
        scratch_shapes=[
            pltpu.VMEM((2, 1536), jnp.int32),
            pltpu.VMEM((32, PART), F32),
            pltpu.VMEM((2, ROWS, 1024), F32),
            pltpu.VMEM((8, 2, ROWS, N), F32),
            pltpu.VMEM((8, 2, ROWS, N), F32),
            pltpu.VMEM((2, 1536, 2 * N), BF16),
            pltpu.VMEM((2, 1536, 2 * N), BF16),
            pltpu.VMEM((1536, 2 * N), F32),
            pltpu.VMEM((1536, N), F32),
            pltpu.VMEM((N, N), F32),
            pltpu.VMEM((TILES * N, N), F32),
            pltpu.VMEM((11, 3, MOST * 32, N), F32),
            pltpu.VMEM((11, 3, MOST * 8, N), F32),
            pltpu.VMEM((11, 4, MOST * 8, N), F32),
            pltpu.VMEM((11, MOST * 32, N), F32),
            pltpu.VMEM((2, TILES * N, N), F32),
            pltpu.VMEM((2, TILES * N, N), F32),
            pltpu.VMEM((4, ROWS, N), F32),
            pltpu.VMEM((4, ROWS, N), F32),
            pltpu.VMEM((8, ROWS, N), F32),
            pltpu.VMEM((1536, 2 * N), BF16),
            pltpu.VMEM((1536, 2 * N), BF16),
            pltpu.VMEM((1536, N), F32),
            pltpu.VMEM((1536, 1536), BF16),
            pltpu.VMEM((1536, 1536), F8),
            pltpu.VMEM((8, N), F32),
            pltpu.VMEM((32, 1536), F32),
            dma((3,)),
            dma((21,)), dma((21,)), dma((24,)), dma((24,)),
            dma((9,)), dma((9,)), dma((4,)), dma((4,)), dma((9,)), dma((9,)),
            dma((33,)), dma((33,)), dma((33,)), dma((33,)), dma((33,)), dma((33,)),
            dma((33,)), dma((33,)), dma((44,)), dma((44,)), dma((44,)), dma((44,)),
        ],
        compiler_params=pltpu.CompilerParams(
            collective_id=0, has_side_effects=True, vmem_limit_bytes=55296 << 10
        ),
        name="whole",
    )(coefs, tilts.T, start_basis.T)
    return block, basis.T


def solution(mesh):
    in_specs = (P(None, "row", "col"), P(), P("col", None))
    out_specs = (P("row", "col"), P("col", None))
    return jax.shard_map(local, mesh=mesh, in_specs=in_specs, out_specs=out_specs, check_vma=False)
```
